32 devices in a mesh: groups: 2 (over y), tp: 4 (over x, core), dp: 4 (over z).
Axes of the slice: x: 2, y: 2, z: 4, core: 2. Of those that a mesh axis runs over, the one named last changes fastest.
Arguments:
- hidden: bfloat16 [128, 2560], P(('groups', 'dp'), 'tp'), parts along dimension 0, may hold values from -40 to 40
- in_gain: float32 [2560], replicated, may hold values from 0.1 to 1.9
- z_weight: bfloat16 [2560, 5120], P(None, 'tp'), may hold values from -0.125 to 0.125
- x_weight: bfloat16 [2560, 5120], P(None, 'tp'), may hold values from -0.125 to 0.125
- bc_weight: bfloat16 [2560, 256], P(None, 'tp'), may hold values from -0.125 to 0.125
- dt_weight: bfloat16 [2560, 80], P(None, 'tp'), may hold values from -0.125 to 0.125
- conv_x_weight: bfloat16 [4, 5120], P(None, 'tp'), may hold values from -3 to 3
- conv_x_bias: bfloat16 [5120], P('tp'), may hold values from -3 to 3
- conv_bc_weight: bfloat16 [4, 256], P(None, 'tp'), may hold values from -3 to 3
- conv_bc_bias: bfloat16 [256], P('tp'), may hold values from -3 to 3
- conv_x_state: bfloat16 [128, 3, 5120], P(('groups', 'dp'), None, 'tp'), parts along dimension 0, may hold values from -6 to 6
- conv_bc_state: bfloat16 [128, 3, 256], P(('groups', 'dp'), None, 'tp'), parts along dimension 0, may hold values from -6 to 6
- dt_bias: float32 [80], P('tp'), may hold values from -4 to -1
- log_rate: float32 [80], P('tp'), may hold values from 0 to 2.5
- skip_gain: float32 [80], P('tp'), may hold values from 0.5 to 2
- ssm_state: float32 [128, 80, 64, 128], P(('groups', 'dp'), 'tp'), parts along dimension 0, may hold values from -20 to 20
- norm_gain: float32 [5120], P('tp'), may hold values from 0.1 to 1.9
- out_weight: bfloat16 [5120, 2560], P('tp'), may hold values from -0.125 to 0.125
- pool_slot: int32 [8, 16], P(('groups', 'dp')), parts along dimension 0, may hold values from 0 to 15, as said below
- active: int32 [128], P(('groups', 'dp')), parts along dimension 0, may hold values 0 or 1
Outputs:
- layer_out: bfloat16 [128, 2560], P(('groups', 'dp'), 'tp'), parts along dimension 0
- conv_x_next: bfloat16 [128, 3, 5120], P(('groups', 'dp'), None, 'tp'), parts along dimension 0
- conv_bc_next: bfloat16 [128, 3, 256], P(('groups', 'dp'), None, 'tp'), parts along dimension 0
- ssm_next: float32 [128, 80, 64, 128], P(('groups', 'dp'), 'tp'), parts along dimension 0
The draws below stay inside these ranges and needn't reach their ends.
There are 2 independent parts, one for each index of `groups`. The reference program is written for one: setup_inputs(seed, part) draws one part's arguments, and reference() takes and returns one part's arrays. A program takes and returns all parts, laid end to end along the dimension named above; an argument that names none is the same for every part. Nothing has to cross between parts.
Inputs may be any that keep to these rules, and one draw needn't show every extreme that they name: `pool_slot`: each row is a permutation of 0 to 15.
All inputs are finite; a program needn't handle non-finite values. No bound on the sum of `active` on one device may be relied on, other than what follows from the above.
Results may differ from the reference program's by a relative error of at most 0.0085.
Values may be sent and summed in bfloat16 or wider, within the bound.
No kernel may reach another device: no remote copies, remote signals or barrier semaphores. Data moves between devices by JAX's collectives and lax.ppermute only.
A program may use at most 128 MiB of HBM per device.

```python
import math
import jax
import jax.numpy as jnp
from jax import lax

D = 2560
HEADS = 80
HP = 64
NS = 128
KW = 4
SEQ_DEV = 16
INNER = 5120
BATCH = 64
N_DP = 4


def draw_hidden(key, part):
    base_key = jax.random.fold_in(key, 21)
    row_key = jax.random.fold_in(key, 22)
    col_key = jax.random.fold_in(key, 23)
    position = jnp.arange(D, dtype=jnp.float32) / (D - 1)
    jitter = jnp.exp(jax.random.uniform(col_key, (D,), jnp.float32, 0.0, math.log(3.3)))
    row_scale = jnp.exp(jax.random.uniform(row_key, (BATCH,), jnp.float32, math.log(0.3), math.log(3.0)))
    base_draw = jnp.clip(jax.random.normal(base_key, (BATCH, D), jnp.float32), -4.0, 4.0)
    col_scale = 3.0 ** position * jitter / 3.3
    return (base_draw * row_scale[:, None] * col_scale[None, :]).astype(jnp.bfloat16)


def draw_ssm_state(key, part):
    base_key = jax.random.fold_in(key, 11)
    head_key = jax.random.fold_in(key, 12)
    position = jnp.arange(HEADS, dtype=jnp.float32) / (HEADS - 1)
    base_draw = jnp.clip(jax.random.normal(base_key, (BATCH, HEADS, HP, NS), jnp.float32), -5.0, 5.0)
    head_trend = 3.0 ** position
    jitter = jnp.exp(jax.random.uniform(head_key, (HEADS,), jnp.float32, 0.0, math.log(3.0)))
    return 0.3 * base_draw * (head_trend * jitter)[None, :, None, None]


def permute_slots(slot_key):
    return jax.random.permutation(slot_key, SEQ_DEV)


def draw_pool_slot(key, part):
    slot_keys = jax.random.split(jax.random.fold_in(key, 31), N_DP)
    return jax.vmap(permute_slots)(slot_keys).astype(jnp.int32)


def place_ends(result, own_key, low, high):
    index_at = [jax.random.randint(jax.random.fold_in(own_key, axis), (), 0, length) for axis, length in enumerate(result.shape)]
    widest = result.shape.index(max(result.shape))
    beside = index_at[:widest] + [(index_at[widest] + 1) % result.shape[widest]] + index_at[widest + 1:]
    return result.at[tuple(index_at)].set(low).at[tuple(beside)].set(high)


def raised(values, own_key, source, target, blocks, factor):
    owner, partner = [(jnp.arange(values.shape[axis_at]) // (values.shape[axis_at] // blocks)).reshape([-1 if axis == axis_at else 1 for axis in range(values.ndim)]) for axis_at in (source, target)]
    chosen = jax.random.permutation(own_key, blocks)[partner]
    strong = (owner == chosen) | (owner == (partner + blocks // 2) % blocks)
    return jnp.where(strong, factor * values, values)


def level_of(stream_key, extent, cuts, least, largest):
    loudness = 1.0
    for axis_at, shards_of in cuts:
        steps = jax.random.uniform(jax.random.fold_in(jax.random.fold_in(stream_key, 6), axis_at), (shards_of,), jnp.float32, least / len(cuts), largest / len(cuts))
        loudness = loudness * jnp.repeat(jnp.exp(steps), extent[axis_at] // shards_of).reshape((-1,) + (1,) * (len(extent) - 1 - axis_at))
    return loudness


def normal_values(rng, dims, scale, bound, pieces=(), kind=jnp.bfloat16):
    entries = jax.random.normal(rng, dims, jnp.float32) * scale
    if len(pieces) > 0:
        entries = level_of(rng, dims, pieces, -0.22, 0.18) * entries
    return jnp.clip(entries, min=-bound, max=bound).astype(kind)


def gaussian_with(stream_key, shape, width, bound, cuts, heavy, kind=jnp.bfloat16):
    result = width * jax.random.normal(stream_key, shape, jnp.float32)
    if cuts:
        result = result * level_of(stream_key, shape, cuts, -0.22, 0.18)
    return jnp.clip(raised(result, jax.random.fold_in(stream_key, 3), *heavy), -bound, bound).astype(kind)


def setup_inputs(seed: int = 0, part: int = 0) -> dict:
    splits = jax.random.split(jax.random.key(seed), 21)
    part_splits = jax.random.split(jax.random.fold_in(splits[20], part), 21)
    hidden = draw_hidden(jax.random.fold_in(jax.random.fold_in(splits[20], part), 71), part)
    in_gain = jnp.clip(1.0 + 0.18 * jax.random.normal(splits[1], (D,), jnp.float32), 0.1, 1.9)
    z_weight = normal_values(splits[2], (D, INNER), D ** -0.5, 0.125, ((1, 4),))
    x_weight = normal_values(splits[3], (D, INNER), D ** -0.5, 0.125, ((1, 4),))
    bc_weight = normal_values(splits[4], (D, 2 * NS), D ** -0.5, 0.125, ((1, 4),))
    dt_weight = normal_values(splits[5], (D, HEADS), D ** -0.5, 0.125, ((1, 4),))
    conv_x_weight = normal_values(splits[6], (KW, INNER), KW ** -0.5, 3.0, ((1, 4),))
    conv_x_bias = normal_values(splits[7], (INNER,), 0.5, 3.0, ((0, 4),))
    conv_bc_weight = normal_values(splits[8], (KW, 2 * NS), KW ** -0.5, 3.0, ((1, 4),))
    conv_bc_bias = normal_values(splits[9], (2 * NS,), 0.5, 3.0, ((0, 4),))
    conv_x_state = normal_values(part_splits[10], (BATCH, KW - 1, INNER), 1.0, 6.0, ((0, 4), (2, 4)))
    conv_bc_state = normal_values(part_splits[11], (BATCH, KW - 1, 2 * NS), 1.0, 6.0, ((0, 4), (2, 4)))
    dt_bias = jnp.clip(-4.0 + 3.0 * jax.random.uniform(splits[12], (HEADS,), jnp.float32) ** level_of(splits[12], (HEADS,), ((0, 4),), -0.2, 0.2), -4.0, -1.0)
    log_rate = jnp.clip(2.5 * jax.random.uniform(splits[13], (HEADS,), jnp.float32) ** level_of(splits[13], (HEADS,), ((0, 4),), -0.2, 0.2), 0.0, 2.5)
    skip_gain = jnp.clip(0.5 + 1.5 * jax.random.uniform(splits[14], (HEADS,), jnp.float32) ** level_of(splits[14], (HEADS,), ((0, 4),), -0.2, 0.2), 0.5, 2.0)
    ssm_state = draw_ssm_state(jax.random.fold_in(jax.random.fold_in(splits[20], part), 71), part)
    norm_gain = jnp.clip(1.0 + 0.18 * jax.random.normal(splits[16], (INNER,), jnp.float32), 0.1, 1.9)
    out_weight = gaussian_with(splits[17], (INNER, D), INNER ** -0.5, 0.125, ((0, 4),), (0, 1, 4, 2.0))
    pool_slot = draw_pool_slot(jax.random.fold_in(jax.random.fold_in(splits[20], part), 71), part)
    active = place_ends((jax.random.randint(part_splits[19], (BATCH,), 0, 4) < 3).astype(jnp.int32), jax.random.fold_in(part_splits[19], 1), 0, 1)
    return dict(hidden=hidden, in_gain=in_gain, z_weight=z_weight, x_weight=x_weight, bc_weight=bc_weight, dt_weight=dt_weight, conv_x_weight=conv_x_weight, conv_x_bias=conv_x_bias, conv_bc_weight=conv_bc_weight, conv_bc_bias=conv_bc_bias, conv_x_state=conv_x_state, conv_bc_state=conv_bc_state, dt_bias=dt_bias, log_rate=log_rate, skip_gain=skip_gain, ssm_state=ssm_state, norm_gain=norm_gain, out_weight=out_weight, pool_slot=pool_slot, active=active)


def convolve(old_state, current, weight, conv_bias):
    window = jnp.concatenate([old_state.astype(jnp.float32), current.astype(jnp.float32)[:, None, :]], axis=1)
    conv_out = lax.optimization_barrier(jnp.sum(window * weight.astype(jnp.float32)[None], axis=1)) + conv_bias.astype(jnp.float32)
    return (jax.nn.silu(conv_out).astype(jnp.bfloat16), window[:, 1:, :].astype(jnp.bfloat16))

def reference(hidden, in_gain, z_weight, x_weight, bc_weight, dt_weight, conv_x_weight, conv_x_bias, conv_bc_weight, conv_bc_bias, conv_x_state, conv_bc_state, dt_bias, log_rate, skip_gain, ssm_state, norm_gain, out_weight, pool_slot, active):
    pool_row = (pool_slot + (jnp.arange(N_DP, dtype=jnp.int32) * SEQ_DEV)[:, None]).reshape(-1).astype(jnp.int32)
    is_live = active > 0
    hidden_f32 = hidden.astype(jnp.float32)
    inv_rms = lax.rsqrt(lax.optimization_barrier(jnp.mean(hidden_f32 * hidden_f32, axis=1, keepdims=True)) + 1e-05)
    normed = (hidden_f32 * inv_rms * in_gain).astype(jnp.bfloat16)
    z_proj = jnp.dot(normed, z_weight, preferred_element_type=jnp.float32).astype(jnp.bfloat16)
    x_proj = jnp.dot(normed, x_weight, preferred_element_type=jnp.float32).astype(jnp.bfloat16)
    bc_proj = jnp.dot(normed, bc_weight, preferred_element_type=jnp.float32).astype(jnp.bfloat16)
    dt_proj = jnp.dot(normed, dt_weight, preferred_element_type=jnp.float32).astype(jnp.bfloat16)
    x_old = conv_x_state[pool_row]
    bc_old = conv_bc_state[pool_row]
    x_conv, x_kept = convolve(x_old, x_proj, conv_x_weight, conv_x_bias)
    bc_conv, bc_kept = convolve(bc_old, bc_proj, conv_bc_weight, conv_bc_bias)
    conv_x_next = conv_x_state.at[pool_row].set(jnp.where(is_live[:, None, None], x_kept, x_old))
    conv_bc_next = conv_bc_state.at[pool_row].set(jnp.where(is_live[:, None, None], bc_kept, bc_old))
    b_rows = bc_conv[:, :NS].astype(jnp.float32)
    c_rows = bc_conv[:, NS:].astype(jnp.float32)
    dt_step = jax.nn.softplus(dt_proj.astype(jnp.float32) + dt_bias)
    decay_rate = jnp.exp(-dt_step * jnp.exp(log_rate))
    x_heads = x_conv.astype(jnp.float32).reshape(BATCH, HEADS, HP)
    old_state = ssm_state[pool_row]
    fresh_state = decay_rate[:, :, None, None] * old_state + (dt_step[:, :, None] * x_heads)[:, :, :, None] * b_rows[:, None, None, :]
    fresh_state = jnp.where(is_live[:, None, None, None], fresh_state, old_state)
    y_heads = jnp.einsum('bhpn,bn->bhp', fresh_state, c_rows, precision=lax.Precision.HIGHEST) + skip_gain[None, :, None] * x_heads
    gated_y = y_heads.reshape(BATCH, INNER) * jax.nn.silu(z_proj.astype(jnp.float32))
    inv_out = lax.rsqrt(lax.optimization_barrier(jnp.mean(gated_y * gated_y, axis=1)) + 1e-05)
    scaled = (gated_y * norm_gain).astype(jnp.bfloat16)
    branch_sum = jnp.dot(scaled, out_weight, preferred_element_type=jnp.float32)
    layer_out = jnp.where(is_live[:, None], (hidden_f32 + inv_out[:, None] * branch_sum).astype(jnp.bfloat16), hidden)
    ssm_next = ssm_state.at[pool_row].set(fresh_state)
    return (layer_out, conv_x_next, conv_bc_next, ssm_next)
```

```python
import functools
import jax
import jax.numpy as jnp
from jax import lax
from jax.experimental import pallas as pl
from jax.experimental.pallas import tpu as pltpu
from jax.sharding import PartitionSpec as P

F32 = jnp.float32
BF16 = jnp.bfloat16
NT = (((1,), (1,)), ((), ()))
TN = (((0,), (0,)), ((), ()))
EPS = 1e-05


def column(row):
    n = row.shape[1]
    eye = lax.broadcasted_iota(jnp.int32, (n, n), 0) == lax.broadcasted_iota(jnp.int32, (n, n), 1)
    return jnp.sum(jnp.where(eye, jnp.broadcast_to(row, (n, n)), jnp.zeros((), row.dtype)), axis=1, keepdims=True)


def silu(v):
    return v * (1.0 / (1.0 + jnp.exp(-v)))


def softplus(v):
    return jnp.maximum(v, 0.0) + jnp.log1p(jnp.exp(-jnp.abs(v)))


def owner_mask(slot_row):
    n = slot_row.shape[1]
    slot_col = column(slot_row.astype(F32))
    return slot_col == lax.broadcasted_iota(jnp.int32, (n, n), 1).astype(F32)


def taps(old, current, weight, bias):
    acc = old[0] * weight[0:1]
    acc = acc + old[1] * weight[1:2]
    acc = acc + old[2] * weight[2:3]
    acc = acc + current * weight[3:4]
    return silu(acc + bias).astype(BF16)


def shift_state(st_ref, newest, live_own, next_ref):
    live_slot = lax.dot_general(live_own, jnp.ones(newest.shape, BF16), TN, preferred_element_type=F32) > 0.5
    at_slot = lax.dot_general(live_own, newest, TN, preferred_element_type=F32)
    for k in range(3):
        newer = st_ref[k + 1].astype(F32) if k < 2 else at_slot
        next_ref[k] = jnp.where(live_slot, newer, st_ref[k].astype(F32)).astype(BF16)


def prep_kernel(count, *refs):
    src, refs = refs[:count], refs[count:]
    (gain_ref, ngain_ref, own_ref, live_own_ref, bcw_ref, dtw_ref, bcst_ref, bcbase_ref, bctap_ref, xst_ref,
     xbase_ref, xtap_ref, dtb_ref, rate_ref, skip_ref, hid_ref, live_ref) = refs[:17]
    slot_s, act_s, bccw_s, bccb_s, xcw_s, xcb_s, sems = refs[17:]
    dst = (gain_ref, ngain_ref, slot_s, act_s, bcw_ref, dtw_ref, bcst_ref, bccw_s, bccb_s, xst_ref, xcw_s, xcb_s,
           dtb_ref, rate_ref, skip_ref, hid_ref)
    copies = [pltpu.make_async_copy(a, b, sems.at[i]) for i, (a, b) in enumerate(zip(src, dst))]
    order = (2, 3, 6, 7, 8, 9, 10, 11, 4, 5, 0, 1, 12, 13, 14, 15)
    for i in order:
        copies[i].start()
    copies[2].wait()
    copies[3].wait()
    own = owner_mask(slot_s[...])
    live = column(act_s[...].astype(F32)) > 0.0
    own_b = own.astype(BF16)
    own_ref[...] = own.astype(F32)
    live_own_ref[...] = (own & live).astype(BF16)
    live_ref[...] = jnp.broadcast_to(live.astype(F32), live_ref.shape)
    for st, cw, cb, base, tap, waits in ((bcst_ref, bccw_s, bccb_s, bcbase_ref, bctap_ref, (6, 7, 8)),
                                         (xst_ref, xcw_s, xcb_s, xbase_ref, xtap_ref, (9, 10, 11))):
        for i in waits:
            copies[i].wait()
        weight = cw[...].astype(F32)
        acc = jnp.broadcast_to(cb[...].astype(F32), base.shape)
        for k in range(3):
            acc = acc + jnp.dot(own_b, st[k], preferred_element_type=F32) * weight[k:k + 1]
        base[...] = acc
        tap[...] = weight[3:4]
    for i in (4, 5, 0, 1, 12, 13, 14, 15):
        copies[i].wait()


def bc_kernel(n, *refs):
    parts, refs = refs[:n], refs[n:]
    gain_ref, own_ref, w_ref, base_ref, tap_ref, normed_ref, bc_ref, proj_ref = refs
    me = lax.axis_index("tp")
    blocks = [p[...] for p in parts]
    width = blocks[0].shape[1]
    for s in range(n):
        pick = blocks[0]
        for k in range(1, n):
            pick = jnp.where(lax.rem(me - k + n, n) == s, blocks[k], pick)
        normed_ref[:, s * width:(s + 1) * width] = pick
    rows = normed_ref[...].astype(F32)
    inv = lax.rsqrt(jnp.mean(rows * rows, axis=1, keepdims=True) + EPS)
    normed = (rows * inv * gain_ref[...]).astype(BF16)
    normed_ref[...] = normed
    proj = lax.dot_general(normed, w_ref[...], NT, preferred_element_type=F32).astype(BF16)
    proj_ref[...] = proj
    bc_ref[...] = silu(base_ref[...] + tap_ref[...] * proj.astype(F32)).astype(BF16)


def in_kernel(hp, normed_ref, xw_ref, zw_ref, dtw_ref, base_ref, tap_ref, dtb_ref, rate_ref, skip_ref, own_ref,
              live_ref, xproj_ref, g1_ref, g2_ref, g3_ref, u_ref, dec_ref):
    normed = normed_ref[...]
    seqs = normed.shape[0]
    chans = xw_ref.shape[1]
    heads = dtw_ref.shape[0]
    live = live_ref[:, :1] > 0.0
    dt = lax.dot_general(normed, dtw_ref[...], NT, preferred_element_type=F32).astype(BF16).astype(F32)
    dt = softplus(dt + dtb_ref[...])
    decay = jnp.exp(-dt * jnp.exp(rate_ref[...]))
    spread = (lax.broadcasted_iota(jnp.int32, (heads, chans), 1) // hp
              == lax.broadcasted_iota(jnp.int32, (heads, chans), 0)).astype(F32)
    wide = jnp.concatenate([dt, decay, jnp.broadcast_to(skip_ref[...], dt.shape)], axis=0)
    wide = jnp.dot(wide, spread, preferred_element_type=F32, precision=lax.Precision.HIGHEST)
    dt_w, dec_w, skip_w = wide[:seqs], wide[seqs:2 * seqs], wide[2 * seqs:]
    kept = jnp.where(live, decay, 1.0)
    kept_slot = lax.dot_general(kept, own_ref[...], TN, preferred_element_type=F32, precision=lax.Precision.HIGHEST)
    for s in range(seqs):
        dec_ref[s] = jnp.broadcast_to(kept_slot[:, s:s + 1], (heads, dec_ref.shape[2]))
    xproj = jnp.dot(normed, xw_ref[...], preferred_element_type=F32).astype(BF16)
    xproj_ref[...] = xproj
    x = silu(base_ref[...] + tap_ref[...] * xproj.astype(F32)).astype(BF16).astype(F32)
    u = dt_w * x
    zproj = jnp.dot(normed, zw_ref[...], preferred_element_type=F32).astype(BF16)
    gate = silu(zproj.astype(F32))
    g1_ref[...] = gate * dec_w
    g2_ref[...] = gate * u
    g3_ref[...] = gate * (skip_w * x)
    u = jnp.where(live, u, 0.0)
    high = u.astype(BF16)
    u_ref[:seqs] = high
    u_ref[seqs:] = (u - high.astype(F32)).astype(BF16)


def out_kernel(n, *refs):
    parts, refs = refs[:n], refs[n:]
    state_ref, own_ref, g1_ref, g2_ref, g3_ref, gain_ref, w_ref = refs[:7]
    sends, (own_sum_ref, bcf_ref, stage) = refs[7:7 + n - 1], refs[7 + n - 1:]
    me = lax.axis_index("tp")
    seqs = g1_ref.shape[0]
    ns = state_ref.shape[2]
    blocks = [p[...] for p in parts]
    width = blocks[0].shape[1]
    for s in range(n):
        pick = blocks[0]
        for k in range(1, n):
            pick = jnp.where(lax.rem(me - k + n, n) == s, blocks[k], pick)
        bcf_ref[:, s * width:(s + 1) * width] = pick
    own = own_ref[...] > 0.5
    b_rows, c_rows = bcf_ref[:, :ns].astype(F32), bcf_ref[:, ns:].astype(F32)
    dot_bc = jnp.sum(b_rows * c_rows, axis=1, keepdims=True)
    y = None
    for s in range(0, seqs, 2):
        pair = [jnp.where(own[:, t:t + 1], c_rows, 0.0).astype(BF16) for t in (s, s + 1)]
        both = jnp.concatenate([state_ref[s].astype(BF16), state_ref[s + 1].astype(BF16)], axis=1)
        term = lax.dot_general(jnp.concatenate(pair, axis=1), both, NT, preferred_element_type=F32)
        y = term if y is None else y + term
    gated = g1_ref[...] * y + g2_ref[...] * dot_bc + g3_ref[...]
    part_sq = jnp.sum(gated * gated, axis=1, keepdims=True)
    scaled = (gated * gain_ref[...]).astype(BF16)
    sq_high = part_sq.astype(BF16).astype(F32)
    width = w_ref.shape[1] // n
    lane = lax.broadcasted_iota(jnp.int32, (seqs, 128), 1)
    tail = jnp.where(lane == 0, sq_high, jnp.where(lane == 1, part_sq - sq_high, 0.0))
    for d in range(n):
        stage[d, :, :width] = jnp.dot(scaled, w_ref[:, d * width:(d + 1) * width], preferred_element_type=F32)
        stage[d, :, width:] = tail
    own_sum_ref[...] = stage[me]
    for k in range(1, n):
        sends[k - 1][...] = stage[lax.rem(me + k, n)].astype(BF16)


def state_kernel(state_ref, u_ref, dec_ref, bcf_ref, own_ref, live_own_ref, xst_ref, xproj_ref, bcst_ref, bcproj_ref,
                 next_ref, xnext_ref, bcnext_ref, ring, sems):
    seqs, chans, ns = state_ref.shape
    heads = dec_ref.shape[1]
    hp = chans // heads
    own = own_ref[...] > 0.5
    b_rows = bcf_ref[:, :ns].astype(F32)
    u_rows = u_ref[...]
    depth = ring.shape[0]

    def copy(s):
        return pltpu.make_async_copy(ring.at[s // 2 % depth], next_ref.at[pl.ds(s, 2)], sems.at[s // 2 % depth])

    for s in range(0, seqs, 2):
        pair = jnp.concatenate([jnp.where(own[:, t:t + 1], b_rows, 0.0).astype(BF16) for t in (s, s + 1)], axis=1)
        fresh = lax.dot_general(u_rows, jnp.concatenate([pair, pair], axis=0), TN, preferred_element_type=F32)
        if s // 2 >= depth:
            copy(s - 2 * depth).wait()
        for t in range(2):
            for h in range(heads):
                rows = slice(h * hp, (h + 1) * hp)
                ring[s // 2 % depth, t, rows, :] = (
                    state_ref[s + t, rows, :] * dec_ref[s + t, h:h + 1, :] + fresh[rows, t * ns:(t + 1) * ns]
                )
        copy(s).start()
    shift_state(xst_ref, xproj_ref[...], live_own_ref[...], xnext_ref)
    shift_state(bcst_ref, bcproj_ref[...], live_own_ref[...], bcnext_ref)
    for s in range(max(0, seqs - 2 * depth), seqs, 2):
        copy(s).wait()


def final_kernel(chans, hid_ref, live_ref, own_ref, *refs):
    got, out_ref = refs[:-1], refs[-1]
    width = hid_ref.shape[1]
    total = own_ref[...]
    for g in got:
        total = total + g[...].astype(F32)
    sq = total[:, width:width + 1] + total[:, width + 1:width + 2]
    inv_out = lax.rsqrt(sq / chans + EPS)
    hidden = hid_ref[...]
    out = (hidden.astype(F32) + inv_out * total[:, :width]).astype(BF16)
    out_ref[...] = jnp.where(live_ref[:, :1] > 0.0, out, hidden)


VM = pl.BlockSpec(memory_space=pltpu.VMEM)
HB = pl.BlockSpec(memory_space=pltpu.HBM)


def call(kernel, name, out, ins, args, outs=None, scratch=(), flops=1e6, moved=1e5, mib=4):
    return pl.pallas_call(
        kernel,
        out_shape=out,
        in_specs=ins,
        out_specs=tuple(outs or [VM] * len(out)),
        scratch_shapes=list(scratch),
        name=name,
        compiler_params=pltpu.CompilerParams(vmem_limit_bytes=mib * 2 ** 20),
        cost_estimate=pl.CostEstimate(flops=int(flops), bytes_accessed=int(moved), transcendentals=0),
    )(*args)


def spread_out(values, n):
    return [lax.ppermute(v, "tp", [(i, (i + k) % n) for i in range(n)]) for k, v in enumerate(values, 1)]


def shards(hidden, in_gain, z_weight, x_weight, bc_weight, dt_weight, conv_x_weight, conv_x_bias, conv_bc_weight,
           conv_bc_bias, conv_x_state, conv_bc_state, dt_bias, log_rate, skip_gain, ssm_state, norm_gain, out_weight,
           pool_slot, active, *, n):
    seqs, heads, hp, ns = ssm_state.shape
    chans = heads * hp
    width = hidden.shape[1]
    bcw = bc_weight.shape[1]
    row = lambda v: v.reshape(1, -1)
    sds = jax.ShapeDtypeStruct
    like = lambda v: sds(v.shape, v.dtype)
    state = ssm_state.reshape(seqs, chans, ns)
    parts = [hidden] + spread_out([hidden] * (n - 1), n)
    src = tuple(pltpu.with_memory_space_constraint(v, pltpu.HBM) for v in (row(in_gain), row(norm_gain), pool_slot.reshape(1, -1), row(active), bc_weight.T, dt_weight.T,
           conv_bc_state.transpose(1, 0, 2), conv_bc_weight, row(conv_bc_bias), conv_x_state.transpose(1, 0, 2),
           conv_x_weight, row(conv_x_bias), row(dt_bias), row(log_rate), row(skip_gain), hidden))
    held = {i: pltpu.VMEM(src[i].shape, src[i].dtype) for i in (2, 3, 7, 8, 10, 11)}
    (gain, ngain, own, live_own, bcw_v, dtw_v, bcst, bcbase, bctap, xst, xbase, xtap, dtb, rate, skip, hid, live) = call(
        functools.partial(prep_kernel, len(src)), "prep",
        (like(src[0]), like(src[1]), sds((seqs, seqs), F32), sds((seqs, seqs), BF16), like(src[4]), like(src[5]),
         like(src[6]), sds((seqs, bcw), F32), sds((1, bcw), F32), like(src[9]), sds((seqs, chans), F32),
         sds((1, chans), F32), like(src[12]), like(src[13]), like(src[14]), like(hidden), sds((seqs, 128), F32)),
        [HB] * len(src), src, scratch=[*held.values(), pltpu.SemaphoreType.DMA((len(src),))], flops=4e6, moved=16e6)
    normed, bc_own, bcproj = call(
        functools.partial(bc_kernel, n), "bc",
        (sds((seqs, n * width), BF16), sds((seqs, bcw), BF16), sds((seqs, bcw), BF16)),
        [VM] * (n + 5), (*parts, gain, own, bcw_v, bcbase, bctap), flops=4e6)
    bc_parts = [bc_own] + spread_out([bc_own] * (n - 1), n)
    wide = sds((seqs, chans), F32)
    xproj, g1, g2, g3, u, dec = call(
        functools.partial(in_kernel, hp), "proj",
        (sds((seqs, chans), BF16), wide, wide, wide, sds((2 * seqs, chans), BF16), sds((seqs, heads, 128), F32)),
        [VM] * 11, (normed, x_weight, z_weight, dtw_v, xbase, xtap, dtb, rate, skip, own, live), flops=2e8, moved=14e6)
    *sends, own_sum, bcf = call(
        functools.partial(out_kernel, n), "out",
        (*[sds((seqs, width + 128), BF16)] * (n - 1), sds((seqs, width + 128), F32), sds((seqs, n * bcw), BF16)),
        [VM] * (n + 7), (*bc_parts, state, own, g1, g2, g3, ngain, out_weight),
        scratch=[pltpu.VMEM((n, seqs, width + 128), F32)], flops=2e8, moved=14e6, mib=12)
    got = spread_out(sends, n)
    fresh, x_next, bc_next = call(
        state_kernel, "state", (like(state), like(xst), like(bcst)), [VM] * 10,
        (state, u, dec, bcf, own, live_own, xst, xproj, bcst, bcproj), outs=(HB, VM, VM),
        scratch=[pltpu.VMEM((4, 2, chans, ns), F32), pltpu.SemaphoreType.DMA((4,))], flops=2e8, moved=14e6, mib=12)
    layer_out, = call(functools.partial(final_kernel, chans * n), "final", (like(hidden),), [VM] * (n + 2),
                      (hid, live, own_sum, *got))
    return (layer_out, x_next.transpose(1, 0, 2), bc_next.transpose(1, 0, 2), fresh.reshape(ssm_state.shape))


def solution(mesh):
    placed = (
        P(("groups", "dp"), "tp"), P(), P(None, "tp"), P(None, "tp"), P(None, "tp"), P(None, "tp"), P(None, "tp"),
        P("tp"), P(None, "tp"), P("tp"), P(("groups", "dp"), None, "tp"), P(("groups", "dp"), None, "tp"), P("tp"),
        P("tp"), P("tp"), P(("groups", "dp"), "tp", None, None), P("tp"), P("tp", None), P(("groups", "dp"), None),
        P(("groups", "dp")),
    )
    return jax.shard_map(
        functools.partial(shards, n=mesh.shape["tp"]),
        mesh=mesh,
        in_specs=placed,
        out_specs=(P(("groups", "dp"), "tp"), P(("groups", "dp"), None, "tp"), P(("groups", "dp"), None, "tp"),
                   P(("groups", "dp"), "tp", None, None)),
        check_vma=False,
    )
```

```python
import functools
import jax
import jax.numpy as jnp
from jax import lax
from jax.experimental import pallas as pl
from jax.experimental.pallas import tpu as pltpu
from jax.sharding import PartitionSpec as P

F32 = jnp.float32
BF16 = jnp.bfloat16
DEPTH = 8
LEAD = 2e10
NT = (((1,), (1,)), ((), ()))
TN = (((0,), (0,)), ((), ()))
EPS = 1e-05


def column(row):
    n = row.shape[1]
    eye = lax.broadcasted_iota(jnp.int32, (n, n), 0) == lax.broadcasted_iota(jnp.int32, (n, n), 1)
    return jnp.sum(jnp.where(eye, jnp.broadcast_to(row, (n, n)), jnp.zeros((), row.dtype)), axis=1, keepdims=True)


def silu(v):
    return v * (1.0 / (1.0 + jnp.exp(-v)))


def softplus(v):
    return jnp.maximum(v, 0.0) + jnp.log1p(jnp.exp(-jnp.abs(v)))


def owner_mask(slot_row):
    n = slot_row.shape[1]
    slot_col = column(slot_row.astype(F32))
    return slot_col == lax.broadcasted_iota(jnp.int32, (n, n), 1).astype(F32)


def taps(old, current, weight, bias):
    acc = old[0] * weight[0:1]
    acc = acc + old[1] * weight[1:2]
    acc = acc + old[2] * weight[2:3]
    acc = acc + current * weight[3:4]
    return silu(acc + bias).astype(BF16)


def shift_state(st_ref, newest, live_own, next_ref):
    live_slot = lax.dot_general(live_own, jnp.ones(newest.shape, BF16), TN, preferred_element_type=F32) > 0.5
    at_slot = lax.dot_general(live_own, newest, TN, preferred_element_type=F32)
    for k in range(3):
        newer = st_ref[k + 1].astype(F32) if k < 2 else at_slot
        next_ref[k] = jnp.where(live_slot, newer, st_ref[k].astype(F32)).astype(BF16)


def load_kernel(src_ref, dst_ref, sem):
    copy = pltpu.make_async_copy(src_ref, dst_ref, sem)
    copy.start()
    copy.wait()


def prep_kernel(count, *refs):
    src, refs = refs[:count], refs[count:]
    (gain_ref, ngain_ref, own_ref, live_own_ref, bcw_ref, dtw_ref, bcst_ref, bcbase_ref, bctap_ref, xst_ref,
     xbase_ref, xtap_ref, dtb_ref, rate_ref, skip_ref, live_ref) = refs[:16]
    gain_s, ngain_s, slot_s, act_s, bccw_s, bccb_s, xcw_s, xcb_s, sems = refs[16:]
    dst = (gain_s, ngain_s, slot_s, act_s, bcw_ref, dtw_ref, bcst_ref, bccw_s, bccb_s, xst_ref, xcw_s, xcb_s,
           dtb_ref, rate_ref, skip_ref)
    copies = [pltpu.make_async_copy(a, b, sems.at[i]) for i, (a, b) in enumerate(zip(src, dst))]
    order = (2, 3, 6, 7, 8, 9, 10, 11, 0, 1, 4, 5, 12, 13, 14)
    for i in order:
        copies[i].start()
    copies[2].wait()
    copies[3].wait()
    own = owner_mask(slot_s[...])
    live = column(act_s[...].astype(F32)) > 0.0
    own_b = own.astype(BF16)
    own_ref[...] = own.astype(F32)
    live_own_ref[...] = (own & live).astype(BF16)
    live_ref[...] = jnp.broadcast_to(live.astype(F32), live_ref.shape)
    for st, cw, cb, base, tap, waits in ((bcst_ref, bccw_s, bccb_s, bcbase_ref, bctap_ref, (6, 7, 8)),
                                         (xst_ref, xcw_s, xcb_s, xbase_ref, xtap_ref, (9, 10, 11))):
        for i in waits:
            copies[i].wait()
        weight = cw[...].astype(F32)
        acc = jnp.broadcast_to(cb[...].astype(F32).reshape(1, -1), base.shape)
        for k in range(3):
            acc = acc + jnp.dot(own_b, st[k], preferred_element_type=F32) * weight[k:k + 1]
        base[...] = acc
        tap[...] = weight[3:4]
    for i in (0, 1):
        copies[i].wait()
    gain_ref[...] = gain_s[...].reshape(1, -1)
    ngain_ref[...] = ngain_s[...].reshape(1, -1)
    for i in (4, 5, 12, 13, 14):
        copies[i].wait()


def bc_kernel(n, *refs):
    parts, refs = refs[:n], refs[n:]
    gain_ref, _, w_ref, base_ref, tap_ref, normed_ref, bc_ref, proj_ref = refs
    me = lax.axis_index("tp")
    blocks = [p[...] for p in parts]
    width = blocks[0].shape[1]
    for s in range(n):
        pick = blocks[0]
        for k in range(1, n):
            pick = jnp.where(lax.rem(me - k + n, n) == s, blocks[k], pick)
        normed_ref[:, s * width:(s + 1) * width] = pick
    rows = normed_ref[...].astype(F32)
    inv = lax.rsqrt(jnp.mean(rows * rows, axis=1, keepdims=True) + EPS)
    normed = (rows * inv * gain_ref[...]).astype(BF16)
    normed_ref[...] = normed
    proj = lax.dot_general(normed, w_ref[...], NT, preferred_element_type=F32).astype(BF16)
    proj_ref[...] = proj
    bc_ref[...] = silu(base_ref[...] + tap_ref[...] * proj.astype(F32)).astype(BF16)


def in_kernel(hp, normed_ref, xw_ref, zw_ref, dtw_ref, base_ref, tap_ref, dtb_ref, rate_ref, skip_ref, own_ref,
              live_ref, ow_ref, xproj_ref, g1_ref, g2_ref, g3_ref, u_ref, dec_ref, owv_ref, sem):
    fetch = pltpu.make_async_copy(ow_ref, owv_ref, sem)
    fetch.start()
    normed = normed_ref[...]
    seqs = normed.shape[0]
    chans = xw_ref.shape[1]
    heads = dtw_ref.shape[0]
    live = live_ref[:, :1] > 0.0
    dt = lax.dot_general(normed, dtw_ref[...], NT, preferred_element_type=F32).astype(BF16).astype(F32)
    dt = softplus(dt + dtb_ref[...])
    decay = jnp.exp(-dt * jnp.exp(rate_ref[...]))
    spread = (lax.broadcasted_iota(jnp.int32, (heads, chans), 1) // hp
              == lax.broadcasted_iota(jnp.int32, (heads, chans), 0)).astype(F32)
    wide = jnp.concatenate([dt, decay, jnp.broadcast_to(skip_ref[...], dt.shape)], axis=0)
    wide = jnp.dot(wide, spread, preferred_element_type=F32, precision=lax.Precision.HIGHEST)
    dt_w, dec_w, skip_w = wide[:seqs], wide[seqs:2 * seqs], wide[2 * seqs:]
    kept = jnp.where(live, decay, 1.0)
    kept_slot = lax.dot_general(kept, own_ref[...], TN, preferred_element_type=F32, precision=lax.Precision.HIGHEST)
    for s in range(seqs):
        dec_ref[s] = jnp.broadcast_to(kept_slot[:, s:s + 1], (heads, dec_ref.shape[2]))
    xproj = jnp.dot(normed, xw_ref[...], preferred_element_type=F32).astype(BF16)
    xproj_ref[...] = xproj
    x = silu(base_ref[...] + tap_ref[...] * xproj.astype(F32)).astype(BF16).astype(F32)
    u = dt_w * x
    zproj = jnp.dot(normed, zw_ref[...], preferred_element_type=F32).astype(BF16)
    gate = silu(zproj.astype(F32))
    g1_ref[...] = gate * dec_w
    g2_ref[...] = gate * u
    g3_ref[...] = gate * (skip_w * x)
    u = jnp.where(live, u, 0.0)
    high = u.astype(BF16)
    low = (u - high.astype(F32)).astype(BF16)
    own_b = own_ref[...].astype(BF16)
    u_slot = (lax.dot_general(own_b, high, TN, preferred_element_type=F32)
              + lax.dot_general(own_b, low, TN, preferred_element_type=F32))
    u_ref[...] = u_slot.T
    fetch.wait()


def out_kernel(n, *refs):
    parts, refs = refs[:n], refs[n:]
    state_ref, own_ref, g1_ref, g2_ref, g3_ref, gain_ref, w_ref = refs[:7]
    sends, (own_sum_ref, bcf_ref, stage) = refs[7:7 + n - 1], refs[7 + n - 1:]
    me = lax.axis_index("tp")
    seqs = g1_ref.shape[0]
    ns = state_ref.shape[2]
    blocks = [p[...] for p in parts]
    width = blocks[0].shape[1]
    for s in range(n):
        pick = blocks[0]
        for k in range(1, n):
            pick = jnp.where(lax.rem(me - k + n, n) == s, blocks[k], pick)
        bcf_ref[:, s * width:(s + 1) * width] = pick
    own = own_ref[...] > 0.5
    b_rows, c_rows = bcf_ref[:, :ns].astype(F32), bcf_ref[:, ns:].astype(F32)
    dot_bc = jnp.sum(b_rows * c_rows, axis=1, keepdims=True)
    y = None
    for s in range(0, seqs, 2):
        pair = [jnp.where(own[:, t:t + 1], c_rows, 0.0).astype(BF16) for t in (s, s + 1)]
        both = jnp.concatenate([state_ref[s].astype(BF16), state_ref[s + 1].astype(BF16)], axis=1)
        term = lax.dot_general(jnp.concatenate(pair, axis=1), both, NT, preferred_element_type=F32)
        y = term if y is None else y + term
    gated = g1_ref[...] * y + g2_ref[...] * dot_bc + g3_ref[...]
    part_sq = jnp.sum(gated * gated, axis=1, keepdims=True)
    scaled = (gated * gain_ref[...]).astype(BF16)
    sq_high = part_sq.astype(BF16).astype(F32)
    width = w_ref.shape[1] // n
    lane = lax.broadcasted_iota(jnp.int32, (seqs, 128), 1)
    tail = jnp.where(lane == 0, sq_high, jnp.where(lane == 1, part_sq - sq_high, 0.0))
    for d in range(n):
        stage[d, :, :width] = jnp.dot(scaled, w_ref[:, d * width:(d + 1) * width], preferred_element_type=F32)
        stage[d, :, width:] = tail
    own_sum_ref[...] = stage[me]
    for k in range(1, n):
        sends[k - 1][...] = stage[lax.rem(me + k, n)].astype(BF16)


def state_kernel(state_ref, u_ref, dec_ref, bcf_ref, own_ref, live_own_ref, xst_ref, xproj_ref, bcst_ref, bcproj_ref,
                 next_ref, xnext_ref, bcnext_ref, ring, xkeep, bckeep, sems, pool_sems):
    seqs, chans, ns = state_ref.shape
    heads = dec_ref.shape[1]
    hp = chans // heads
    b_slot = lax.dot_general(own_ref[...].astype(BF16), bcf_ref[:, :ns], TN, preferred_element_type=F32)
    depth = ring.shape[0]

    def copy(s):
        return pltpu.make_async_copy(ring.at[s % depth], next_ref.at[s], sems.at[s % depth])

    for s in range(seqs):
        if s >= depth:
            copy(s - depth).wait()
        for h in range(heads):
            rows = slice(h * hp, (h + 1) * hp)
            ring[s % depth, rows, :] = (
                state_ref[s, rows, :] * dec_ref[s, h:h + 1, :] + u_ref[rows, s:s + 1] * b_slot[s:s + 1]
            )
        copy(s).start()
        if s == seqs // 4:
            shift_state(xst_ref, xproj_ref[...], live_own_ref[...], xkeep)
            shift_state(bcst_ref, bcproj_ref[...], live_own_ref[...], bckeep)
            pools = [pltpu.make_async_copy(xkeep, xnext_ref, pool_sems.at[0]),
                     pltpu.make_async_copy(bckeep, bcnext_ref, pool_sems.at[1])]
            for pool in pools:
                pool.start()
    for s in range(max(0, seqs - depth), seqs):
        copy(s).wait()
    for pool in pools:
        pool.wait()


def final_kernel(chans, hid_ref, live_ref, own_ref, *refs):
    got, out_ref = refs[:-1], refs[-1]
    width = hid_ref.shape[1]
    total = own_ref[...]
    for g in got:
        total = total + g[...].astype(F32)
    sq = total[:, width:width + 1] + total[:, width + 1:width + 2]
    inv_out = lax.rsqrt(sq / chans + EPS)
    hidden = hid_ref[...]
    out = (hidden.astype(F32) + inv_out * total[:, :width]).astype(BF16)
    out_ref[...] = jnp.where(live_ref[:, :1] > 0.0, out, hidden)


VM = pl.BlockSpec(memory_space=pltpu.VMEM)
HB = pl.BlockSpec(memory_space=pltpu.HBM)


def call(kernel, name, out, ins, args, outs=None, scratch=(), flops=1e6, moved=1e5, mib=4):
    return pl.pallas_call(
        kernel,
        out_shape=out,
        in_specs=ins,
        out_specs=tuple(outs or [VM] * len(out)),
        scratch_shapes=list(scratch),
        name=name,
        compiler_params=pltpu.CompilerParams(vmem_limit_bytes=mib * 2 ** 20),
        cost_estimate=pl.CostEstimate(flops=int(flops), bytes_accessed=int(moved), transcendentals=0),
    )(*args)


def spread_out(values, n):
    return [lax.ppermute(v, "tp", [(i, (i + k) % n) for i in range(n)]) for k, v in enumerate(values, 1)]


def shards(hidden, in_gain, z_weight, x_weight, bc_weight, dt_weight, conv_x_weight, conv_x_bias, conv_bc_weight,
           conv_bc_bias, conv_x_state, conv_bc_state, dt_bias, log_rate, skip_gain, ssm_state, norm_gain, out_weight,
           pool_slot, active, *, n):
    seqs, heads, hp, ns = ssm_state.shape
    chans = heads * hp
    width = hidden.shape[1]
    bcw = bc_weight.shape[1]
    row = lambda v: v.reshape(1, -1)
    pinned = lambda v: pltpu.with_memory_space_constraint(v, pltpu.HBM)
    sds = jax.ShapeDtypeStruct
    like = lambda v: sds(v.shape, v.dtype)
    state = ssm_state.reshape(seqs, chans, ns)
    hid, = call(load_kernel, "load", (like(hidden),), [HB], (pinned(hidden),), scratch=[pltpu.SemaphoreType.DMA],
                flops=LEAD, moved=1e5)
    parts = [hid] + spread_out([hid] * (n - 1), n)
    src = (in_gain, norm_gain, row(pool_slot), row(active), bc_weight.T, dt_weight.T, conv_bc_state.transpose(1, 0, 2),
           conv_bc_weight, row(conv_bc_bias), conv_x_state.transpose(1, 0, 2), conv_x_weight, conv_x_bias, row(dt_bias),
           row(log_rate), row(skip_gain))
    held = {i: pltpu.VMEM(src[i].shape, src[i].dtype) for i in (0, 1, 2, 3, 7, 8, 10, 11)}
    (gain, ngain, own, live_own, bcw_v, dtw_v, bcst, bcbase, bctap, xst, xbase, xtap, dtb, rate, skip, live) = call(
        functools.partial(prep_kernel, len(src)), "prep",
        (like(row(in_gain)), like(row(norm_gain)), sds((seqs, seqs), F32), sds((seqs, seqs), BF16), like(src[4]), like(src[5]),
         like(src[6]), sds((seqs, bcw), F32), sds((1, bcw), F32), like(src[9]), sds((seqs, chans), F32),
         sds((1, chans), F32), like(src[12]), like(src[13]), like(src[14]), sds((seqs, 128), F32)),
        [HB] * len(src), tuple(map(pinned, src)), scratch=[*held.values(), pltpu.SemaphoreType.DMA((len(src),))], flops=4e6, moved=1e6)
    normed, bc_own, bcproj = call(
        functools.partial(bc_kernel, n), "bc",
        (sds((seqs, n * width), BF16), sds((seqs, bcw), BF16), sds((seqs, bcw), BF16)),
        [VM] * (n + 5), (*parts, gain, state, bcw_v, bcbase, bctap), flops=4e6)
    bc_parts = [bc_own] + spread_out([bc_own] * (n - 1), n)
    wide = sds((seqs, chans), F32)
    xproj, g1, g2, g3, u, dec, out_w = call(
        functools.partial(in_kernel, hp), "proj",
        (sds((seqs, chans), BF16), wide, wide, wide, sds((chans, seqs), F32), sds((seqs, heads, 128), F32),
         like(out_weight)),
        [VM] * 11 + [HB], (normed, x_weight, z_weight, dtw_v, xbase, xtap, dtb, rate, skip, own, live, pinned(out_weight)),
        scratch=[pltpu.SemaphoreType.DMA], flops=1e6, moved=1e5)
    *sends, own_sum, bcf = call(
        functools.partial(out_kernel, n), "out",
        (*[sds((seqs, width + 128), BF16)] * (n - 1), sds((seqs, width + 128), F32), sds((seqs, n * bcw), BF16)),
        [VM] * (n + 7), (*bc_parts, state, own, g1, g2, g3, ngain, out_w),
        scratch=[pltpu.VMEM((n, seqs, width + 128), F32)], flops=2e8, moved=14e6, mib=12)
    got = spread_out(sends, n)
    fresh, x_next, bc_next = call(
        state_kernel, "state", (like(state), like(xst), like(bcst)), [VM] * 10,
        (state, u, dec, bcf, own, live_own, xst, xproj, bcst, bcproj), outs=(HB, HB, HB),
        scratch=[pltpu.VMEM((DEPTH, chans, ns), F32), pltpu.VMEM(xst.shape, BF16), pltpu.VMEM(bcst.shape, BF16),
                 pltpu.SemaphoreType.DMA((DEPTH,)), pltpu.SemaphoreType.DMA((2,))], flops=2e8, moved=14e6, mib=12)
    layer_out, = call(functools.partial(final_kernel, chans * n), "final", (like(hidden),), [VM] * (n + 2),
                      (hid, live, own_sum, *got))
    return (layer_out, x_next.transpose(1, 0, 2), bc_next.transpose(1, 0, 2), fresh.reshape(ssm_state.shape))


def solution(mesh):
    placed = (
        P(("groups", "dp"), "tp"), P(), P(None, "tp"), P(None, "tp"), P(None, "tp"), P(None, "tp"), P(None, "tp"),
        P("tp"), P(None, "tp"), P("tp"), P(("groups", "dp"), None, "tp"), P(("groups", "dp"), None, "tp"), P("tp"),
        P("tp"), P("tp"), P(("groups", "dp"), "tp", None, None), P("tp"), P("tp", None), P(("groups", "dp"), None),
        P(("groups", "dp")),
    )
    return jax.shard_map(
        functools.partial(shards, n=mesh.shape["tp"]),
        mesh=mesh,
        in_specs=placed,
        out_specs=(P(("groups", "dp"), "tp"), P(("groups", "dp"), None, "tp"), P(("groups", "dp"), None, "tp"),
                   P(("groups", "dp"), "tp", None, None)),
        check_vma=False,
    )
```

```python
import functools
import jax
import jax.numpy as jnp
from jax import lax
from jax.experimental import pallas as pl
from jax.experimental.pallas import tpu as pltpu
from jax.sharding import PartitionSpec as P

F32 = jnp.float32
BF16 = jnp.bfloat16
LEAD = 2e10
NT = (((1,), (1,)), ((), ()))
TN = (((0,), (0,)), ((), ()))
EPS = 1e-05


def column(row):
    n = row.shape[1]
    eye = lax.broadcasted_iota(jnp.int32, (n, n), 0) == lax.broadcasted_iota(jnp.int32, (n, n), 1)
    return jnp.sum(jnp.where(eye, jnp.broadcast_to(row, (n, n)), jnp.zeros((), row.dtype)), axis=1, keepdims=True)


def silu(v):
    return v * (1.0 / (1.0 + jnp.exp(-v)))


def softplus(v):
    return jnp.maximum(v, 0.0) + jnp.log1p(jnp.exp(-jnp.abs(v)))


def owner_mask(slot_row):
    n = slot_row.shape[1]
    slot_col = column(slot_row.astype(F32))
    return slot_col == lax.broadcasted_iota(jnp.int32, (n, n), 1).astype(F32)


def taps(old, current, weight, bias):
    acc = old[0] * weight[0:1]
    acc = acc + old[1] * weight[1:2]
    acc = acc + old[2] * weight[2:3]
    acc = acc + current * weight[3:4]
    return silu(acc + bias).astype(BF16)


def shift_state(st_ref, newest, live_own, next_ref):
    live_slot = lax.dot_general(live_own, jnp.ones(newest.shape, BF16), TN, preferred_element_type=F32) > 0.5
    at_slot = lax.dot_general(live_own, newest, TN, preferred_element_type=F32)
    for k in range(3):
        newer = st_ref[k + 1].astype(F32) if k < 2 else at_slot
        next_ref[k] = jnp.where(live_slot, newer, st_ref[k].astype(F32)).astype(BF16)


def load_kernel(src_ref, dst_ref, sem):
    copy = pltpu.make_async_copy(src_ref, dst_ref, sem)
    copy.start()
    copy.wait()


def prep_kernel(count, *refs):
    src, refs = refs[:count], refs[count:]
    (gain_ref, ngain_ref, own_ref, live_own_ref, bcw_ref, dtw_ref, bcst_ref, bcbase_ref, bctap_ref, xst_ref,
     xbase_ref, xtap_ref, dtb_ref, rate_ref, skip_ref, live_ref) = refs[:16]
    gain_s, ngain_s, slot_s, act_s, bccw_s, bccb_s, xcw_s, xcb_s, sems = refs[16:]
    dst = (gain_s, ngain_s, slot_s, act_s, bcw_ref, dtw_ref, bcst_ref, bccw_s, bccb_s, xst_ref, xcw_s, xcb_s,
           dtb_ref, rate_ref, skip_ref)
    copies = [pltpu.make_async_copy(a, b, sems.at[i]) for i, (a, b) in enumerate(zip(src, dst))]
    order = (2, 3, 6, 7, 8, 9, 10, 11, 0, 1, 4, 5, 12, 13, 14)
    for i in order:
        copies[i].start()
    copies[2].wait()
    copies[3].wait()
    own = owner_mask(slot_s[...])
    live = column(act_s[...].astype(F32)) > 0.0
    own_b = own.astype(BF16)
    own_ref[...] = own.astype(F32)
    live_own_ref[...] = (own & live).astype(BF16)
    live_ref[...] = jnp.broadcast_to(live.astype(F32), live_ref.shape)
    for st, cw, cb, base, tap, waits in ((bcst_ref, bccw_s, bccb_s, bcbase_ref, bctap_ref, (6, 7, 8)),
                                         (xst_ref, xcw_s, xcb_s, xbase_ref, xtap_ref, (9, 10, 11))):
        for i in waits:
            copies[i].wait()
        weight = cw[...].astype(F32)
        acc = jnp.broadcast_to(cb[...].astype(F32).reshape(1, -1), base.shape)
        for k in range(3):
            acc = acc + jnp.dot(own_b, st[k], preferred_element_type=F32) * weight[k:k + 1]
        base[...] = acc
        tap[...] = weight[3:4]
    for i in (0, 1):
        copies[i].wait()
    gain_ref[...] = gain_s[...].reshape(1, -1)
    ngain_ref[...] = ngain_s[...].reshape(1, -1)
    for i in (4, 5, 12, 13, 14):
        copies[i].wait()


def bc_kernel(n, *refs):
    parts, refs = refs[:n], refs[n:]
    gain_ref, bcw_ref, dtw_ref, base_ref, tap_ref, normed_ref, bc_ref, proj_ref, dt_ref = refs
    bcw, heads = bc_ref.shape[1], dt_ref.shape[1]
    me = lax.axis_index("tp")
    blocks = [p[...] for p in parts]
    width = blocks[0].shape[1]
    for s in range(n):
        pick = blocks[0]
        for k in range(1, n):
            pick = jnp.where(source(me, k, n) == s, blocks[k], pick)
        normed_ref[:, s * width:(s + 1) * width] = pick
    rows = normed_ref[...].astype(F32)
    inv = lax.rsqrt(jnp.mean(rows * rows, axis=1, keepdims=True) + EPS)
    normed = (rows * inv * gain_ref[...]).astype(BF16)
    normed_ref[...] = normed
    side = jnp.concatenate([bcw_ref[...], dtw_ref[...]], axis=0)
    both = lax.dot_general(normed, side, NT, preferred_element_type=F32).astype(BF16)
    dt_ref[...] = both[:, bcw:bcw + heads].astype(F32)
    proj = both[:, :bcw]
    proj_ref[...] = proj
    bc_ref[...] = silu(base_ref[...] + tap_ref[...] * proj.astype(F32)).astype(BF16)


def terms(v):
    high = v.astype(BF16)
    rest = v - high.astype(F32)
    mid = rest.astype(BF16)
    return jnp.concatenate([high, mid, (rest - mid.astype(F32)).astype(BF16)], axis=0)


def in_kernel(hp, _, normed_ref, xw_ref, zw_ref, base_ref, tap_ref, dt_ref, dtb_ref, rate_ref, skip_ref, own_ref,
              live_ref, xproj_ref, g1_ref, g2_ref, g3_ref, u_ref, dec_ref):
    normed = normed_ref[...]
    xproj = jnp.dot(normed, xw_ref[...], preferred_element_type=F32).astype(BF16)
    xproj_ref[...] = xproj
    seqs, heads = dt_ref.shape
    chans = xw_ref.shape[1]
    live = live_ref[:, :1] > 0.0
    dt = softplus(dt_ref[...] + dtb_ref[...])
    decay = jnp.exp(-dt * jnp.exp(rate_ref[...]))
    spread = (lax.broadcasted_iota(jnp.int32, (heads, chans), 1) // hp
              == lax.broadcasted_iota(jnp.int32, (heads, chans), 0)).astype(BF16)
    rows = 2 * seqs + 16
    wide = jnp.concatenate([dt, decay, jnp.broadcast_to(skip_ref[...], (16, heads))], axis=0)
    wide = jnp.dot(terms(wide), spread, preferred_element_type=F32)
    wide = wide[:rows] + wide[rows:2 * rows] + wide[2 * rows:]
    dt_w, dec_w, skip_w = wide[:seqs], wide[seqs:2 * seqs], wide[2 * seqs:2 * seqs + 1]
    own_b = own_ref[...].astype(BF16)
    kept = lax.dot_general(terms(jnp.where(live, decay, 1.0)), jnp.concatenate([own_b] * 3, axis=0), TN,
                           preferred_element_type=F32)
    for s in range(seqs):
        dec_ref[s] = jnp.broadcast_to(kept[:, s:s + 1], (heads, dec_ref.shape[2]))
    x = silu(base_ref[...] + tap_ref[...] * xproj.astype(F32)).astype(BF16).astype(F32)
    u = dt_w * x
    live_u = jnp.where(live, u, 0.0)
    high = live_u.astype(BF16)
    u_slot = lax.dot_general(jnp.concatenate([own_b, own_b], axis=0),
                             jnp.concatenate([high, (live_u - high.astype(F32)).astype(BF16)], axis=0), TN,
                             preferred_element_type=F32)
    u_ref[...] = u_slot.T
    zproj = jnp.dot(normed, zw_ref[...], preferred_element_type=F32).astype(BF16)
    gate = silu(zproj.astype(F32))
    g1_ref[...] = gate * dec_w
    g2_ref[...] = gate * u
    g3_ref[...] = gate * (skip_w * x)


def early(seqs):
    return range(0, seqs, 2)


def step_slot(s, dst, state_ref, u_ref, dec_ref, b_slot):
    heads = dec_ref.shape[1]
    hp = state_ref.shape[1] // heads
    for h in range(heads):
        rows = slice(h * hp, (h + 1) * hp)
        dst[rows, :] = state_ref[s, rows, :] * dec_ref[s, h:h + 1, :] + u_ref[rows, s:s + 1] * b_slot[s:s + 1]


def out_kernel(n, *refs):
    parts, refs = refs[:n], refs[n:]
    state_ref, own_ref, g1_ref, g2_ref, g3_ref, gain_ref, w_ref, u_ref, dec_ref = refs[:9]
    sends, (own_sum_ref, bcf_ref, next_ref, stage, ring, sems) = refs[9:9 + n - 1], refs[9 + n - 1:]
    me = lax.axis_index("tp")
    seqs = g1_ref.shape[0]
    ns = state_ref.shape[2]
    blocks = [p[...] for p in parts]
    width = blocks[0].shape[1]
    for s in range(n):
        pick = blocks[0]
        for k in range(1, n):
            pick = jnp.where(source(me, k, n) == s, blocks[k], pick)
        bcf_ref[:, s * width:(s + 1) * width] = pick
    own = own_ref[...] > 0.5
    b_rows, c_rows = bcf_ref[:, :ns].astype(F32), bcf_ref[:, ns:].astype(F32)
    dot_bc = jnp.sum(b_rows * c_rows, axis=1, keepdims=True)
    b_slot = lax.dot_general(own_ref[...].astype(BF16), bcf_ref[:, :ns], TN, preferred_element_type=F32)
    y, copies = None, []
    for s in range(0, seqs, 2):
        if s in early(seqs):
            at = len(copies)
            step_slot(s, ring.at[at], state_ref, u_ref, dec_ref, b_slot)
            copies.append(pltpu.make_async_copy(ring.at[at], next_ref.at[s], sems.at[at]))
            copies[-1].start()
        pair = [jnp.where(own[:, t:t + 1], c_rows, 0.0).astype(BF16) for t in (s, s + 1)]
        both = jnp.concatenate([state_ref[s].astype(BF16), state_ref[s + 1].astype(BF16)], axis=1)
        term = lax.dot_general(jnp.concatenate(pair, axis=1), both, NT, preferred_element_type=F32)
        y = term if y is None else y + term
    gated = g1_ref[...] * y + g2_ref[...] * dot_bc + g3_ref[...]
    part_sq = jnp.sum(gated * gated, axis=1, keepdims=True)
    scaled = (gated * gain_ref[...]).astype(BF16)
    sq_high = part_sq.astype(BF16).astype(F32)
    width = w_ref.shape[1] // n
    lane = lax.broadcasted_iota(jnp.int32, (seqs, 128), 1)
    tail = jnp.where(lane == 0, sq_high, jnp.where(lane == 1, part_sq - sq_high, 0.0))
    for d in range(n):
        stage[d, :, :width] = jnp.dot(scaled, w_ref[:, d * width:(d + 1) * width], preferred_element_type=F32)
        stage[d, :, width:] = tail
    own_sum_ref[...] = stage[me]
    for k in range(1, n):
        sends[k - 1][...] = stage[partner(me, k, n)].astype(BF16)
    for copy in copies:
        copy.wait()


def state_kernel(_, state_ref, u_ref, dec_ref, bcf_ref, own_ref, live_own_ref, xst_ref, xproj_ref, bcst_ref, bcproj_ref,
                 next_ref, xnext_ref, bcnext_ref, ring, xkeep, bckeep, sems, pool_sems):
    seqs, chans, ns = state_ref.shape
    b_slot = lax.dot_general(own_ref[...].astype(BF16), bcf_ref[:, :ns], TN, preferred_element_type=F32)
    late = [s for s in range(seqs) if s not in early(seqs)]
    copies = []
    for at, s in enumerate(late):
        step_slot(s, ring.at[at], state_ref, u_ref, dec_ref, b_slot)
        copies.append(pltpu.make_async_copy(ring.at[at], next_ref.at[s], sems.at[at]))
        copies[-1].start()
        if at == len(late) // 2:
            shift_state(xst_ref, xproj_ref[...], live_own_ref[...], xkeep)
            shift_state(bcst_ref, bcproj_ref[...], live_own_ref[...], bckeep)
            pools = [pltpu.make_async_copy(xkeep, xnext_ref, pool_sems.at[0]),
                     pltpu.make_async_copy(bckeep, bcnext_ref, pool_sems.at[1])]
            for pool in pools:
                pool.start()
    for copy in copies + pools:
        copy.wait()


def final_kernel(chans, hid_ref, live_ref, own_ref, *refs):
    got, out_ref = refs[:-1], refs[-1]
    width = hid_ref.shape[1]
    total = own_ref[...]
    for g in got:
        total = total + g[...].astype(F32)
    sq = total[:, width:width + 1] + total[:, width + 1:width + 2]
    inv_out = lax.rsqrt(sq / chans + EPS)
    hidden = hid_ref[...]
    out = (hidden.astype(F32) + inv_out * total[:, :width]).astype(BF16)
    out_ref[...] = jnp.where(live_ref[:, :1] > 0.0, out, hidden)


VM = pl.BlockSpec(memory_space=pltpu.VMEM)
HB = pl.BlockSpec(memory_space=pltpu.HBM)


def call(kernel, name, out, ins, args, outs=None, scratch=(), flops=1e6, moved=1e5, mib=4, alias=None):
    return pl.pallas_call(
        kernel,
        out_shape=out,
        in_specs=ins,
        out_specs=tuple(outs or [VM] * len(out)),
        scratch_shapes=list(scratch),
        input_output_aliases=alias or {},
        name=name,
        compiler_params=pltpu.CompilerParams(vmem_limit_bytes=mib * 2 ** 20),
        cost_estimate=pl.CostEstimate(flops=int(flops), bytes_accessed=int(moved), transcendentals=0),
    )(*args)


def partner(i, k, n):
    return i ^ k if n & (n - 1) == 0 else lax.rem(i + k, n)


def source(i, k, n):
    return i ^ k if n & (n - 1) == 0 else lax.rem(i - k + n, n)


def spread_out(values, n):
    pairs = n & (n - 1) == 0
    return [lax.ppermute(v, "tp", [(i, i ^ k if pairs else (i + k) % n) for i in range(n)])
            for k, v in enumerate(values, 1)]


def shards(hidden, in_gain, z_weight, x_weight, bc_weight, dt_weight, conv_x_weight, conv_x_bias, conv_bc_weight,
           conv_bc_bias, conv_x_state, conv_bc_state, dt_bias, log_rate, skip_gain, ssm_state, norm_gain, out_weight,
           pool_slot, active, *, n):
    seqs, heads, hp, ns = ssm_state.shape
    chans = heads * hp
    width = hidden.shape[1]
    bcw = bc_weight.shape[1]
    row = lambda v: v.reshape(1, -1)
    pinned = lambda v: pltpu.with_memory_space_constraint(v, pltpu.HBM)
    sds = jax.ShapeDtypeStruct
    like = lambda v: sds(v.shape, v.dtype)
    state = ssm_state.reshape(seqs, chans, ns)
    hid, = call(load_kernel, "load", (like(hidden),), [HB], (pinned(hidden),), scratch=[pltpu.SemaphoreType.DMA],
                flops=LEAD, moved=1e5)
    parts = [hid] + spread_out([hid] * (n - 1), n)
    src = (in_gain, norm_gain, row(pool_slot), row(active), bc_weight.T, dt_weight.T, conv_bc_state.transpose(1, 0, 2),
           conv_bc_weight, row(conv_bc_bias), conv_x_state.transpose(1, 0, 2), conv_x_weight, conv_x_bias, row(dt_bias),
           row(log_rate), row(skip_gain))
    held = {i: pltpu.VMEM(src[i].shape, src[i].dtype) for i in (0, 1, 2, 3, 7, 8, 10, 11)}
    (gain, ngain, own, live_own, bcw_v, dtw_v, bcst, bcbase, bctap, xst, xbase, xtap, dtb, rate, skip, live) = call(
        functools.partial(prep_kernel, len(src)), "prep",
        (like(row(in_gain)), like(row(norm_gain)), sds((seqs, seqs), F32), sds((seqs, seqs), BF16), like(src[4]), like(src[5]),
         like(src[6]), sds((seqs, bcw), F32), sds((1, bcw), F32), like(src[9]), sds((seqs, chans), F32),
         sds((1, chans), F32), like(src[12]), like(src[13]), like(src[14]), sds((seqs, 128), F32)),
        [HB] * len(src), tuple(map(pinned, src)), scratch=[*held.values(), pltpu.SemaphoreType.DMA((len(src),))], flops=4e6, moved=1e6)
    normed, bc_own, bcproj, dt = call(
        functools.partial(bc_kernel, n), "bc",
        (sds((seqs, n * width), BF16), sds((seqs, bcw), BF16), sds((seqs, bcw), BF16),
         sds((seqs, heads), F32)),
        [VM] * (n + 5), (*parts, gain, bcw_v, dtw_v, bcbase, bctap), flops=4e6)
    bc_parts = [bc_own] + spread_out([bc_own] * (n - 1), n)
    wide = sds((seqs, chans), F32)
    xproj, g1, g2, g3, u, dec = call(
        functools.partial(in_kernel, hp), "proj",
        (sds((seqs, chans), BF16), wide, wide, wide, sds((chans, seqs), F32), sds((seqs, heads, 128), F32)),
        [VM] * 12, (state, normed, x_weight, z_weight, xbase, xtap, dt, dtb, rate, skip, own, live))
    count = len(early(seqs))
    *sends, own_sum, bcf, begun = call(
        functools.partial(out_kernel, n), "out",
        (*[sds((seqs, width + 128), BF16)] * (n - 1), sds((seqs, width + 128), F32), sds((seqs, n * bcw), BF16),
         like(state)),
        [VM] * (n + 9), (*bc_parts, state, own, g1, g2, g3, ngain, out_weight, u, dec), outs=(VM,) * (n + 1) + (HB,),
        scratch=[pltpu.VMEM((n, seqs, width + 128), F32), pltpu.VMEM((count, chans, ns), F32),
                 pltpu.SemaphoreType.DMA((count,))], flops=2e8, moved=14e6, mib=12)
    got = spread_out(sends, n)
    fresh, x_next, bc_next = call(
        state_kernel, "state", (like(state), like(xst), like(bcst)), [HB] + [VM] * 10,
        (begun, state, u, dec, bcf, own, live_own, xst, xproj, bcst, bcproj), outs=(HB, HB, HB),
        scratch=[pltpu.VMEM((seqs - count, chans, ns), F32), pltpu.VMEM(xst.shape, BF16), pltpu.VMEM(bcst.shape, BF16),
                 pltpu.SemaphoreType.DMA((seqs - count,)), pltpu.SemaphoreType.DMA((2,))], flops=2e8, moved=14e6, mib=12,
        alias={0: 0})
    layer_out, = call(functools.partial(final_kernel, chans * n), "final", (like(hidden),), [VM] * (n + 2),
                      (hid, live, own_sum, *got))
    return (layer_out, x_next.transpose(1, 0, 2), bc_next.transpose(1, 0, 2), fresh.reshape(ssm_state.shape))


def solution(mesh):
    placed = (
        P(("groups", "dp"), "tp"), P(), P(None, "tp"), P(None, "tp"), P(None, "tp"), P(None, "tp"), P(None, "tp"),
        P("tp"), P(None, "tp"), P("tp"), P(("groups", "dp"), None, "tp"), P(("groups", "dp"), None, "tp"), P("tp"),
        P("tp"), P("tp"), P(("groups", "dp"), "tp", None, None), P("tp"), P("tp", None), P(("groups", "dp"), None),
        P(("groups", "dp")),
    )
    return jax.shard_map(
        functools.partial(shards, n=mesh.shape["tp"]),
        mesh=mesh,
        in_specs=placed,
        out_specs=(P(("groups", "dp"), "tp"), P(("groups", "dp"), None, "tp"), P(("groups", "dp"), None, "tp"),
                   P(("groups", "dp"), "tp", None, None)),
        check_vma=False,
    )
```

```python
import functools
import jax
import jax.numpy as jnp
from jax import lax
from jax.experimental import pallas as pl
from jax.experimental.pallas import tpu as pltpu
from jax.sharding import PartitionSpec as P

F32 = jnp.float32
BF16 = jnp.bfloat16
LEAD = 2e10
NT = (((1,), (1,)), ((), ()))
TN = (((0,), (0,)), ((), ()))
EPS = 1e-05


def column(row):
    n = row.shape[1]
    eye = lax.broadcasted_iota(jnp.int32, (n, n), 0) == lax.broadcasted_iota(jnp.int32, (n, n), 1)
    return jnp.sum(jnp.where(eye, jnp.broadcast_to(row, (n, n)), jnp.zeros((), row.dtype)), axis=1, keepdims=True)


def silu(v):
    return v * (1.0 / (1.0 + jnp.exp(-v)))


def softplus(v):
    return jnp.maximum(v, 0.0) + jnp.log1p(jnp.exp(-jnp.abs(v)))


def owner_mask(slot_row):
    n = slot_row.shape[1]
    slot_col = column(slot_row.astype(F32))
    return slot_col == lax.broadcasted_iota(jnp.int32, (n, n), 1).astype(F32)


def taps(old, current, weight, bias):
    acc = old[0] * weight[0:1]
    acc = acc + old[1] * weight[1:2]
    acc = acc + old[2] * weight[2:3]
    acc = acc + current * weight[3:4]
    return silu(acc + bias).astype(BF16)


def shift_state(st_ref, newest, live_own, next_ref):
    live_slot = lax.dot_general(live_own, jnp.ones(newest.shape, BF16), TN, preferred_element_type=F32) > 0.5
    at_slot = lax.dot_general(live_own, newest, TN, preferred_element_type=F32)
    for k in range(3):
        newer = st_ref[k + 1].astype(F32) if k < 2 else at_slot
        next_ref[k] = jnp.where(live_slot, newer, st_ref[k].astype(F32)).astype(BF16)


def load_kernel(src_ref, dst_ref, sem):
    copy = pltpu.make_async_copy(src_ref, dst_ref, sem)
    copy.start()
    copy.wait()


def prep_kernel(count, *refs):
    src, refs = refs[:count], refs[count:]
    (gain_ref, ngain_ref, own_ref, live_own_ref, bcw_ref, dtw_ref, bcst_ref, bcbase_ref, bctap_ref, xst_ref,
     xbase_ref, xtap_ref, dtb_ref, rate_ref, skip_ref, live_ref) = refs[:16]
    gain_s, ngain_s, slot_s, act_s, bccw_s, bccb_s, xcw_s, xcb_s, sems = refs[16:]
    dst = (gain_s, ngain_s, slot_s, act_s, bcw_ref, dtw_ref, bcst_ref, bccw_s, bccb_s, xst_ref, xcw_s, xcb_s,
           dtb_ref, rate_ref, skip_ref)
    copies = [pltpu.make_async_copy(a, b, sems.at[i]) for i, (a, b) in enumerate(zip(src, dst))]
    order = (2, 3, 6, 7, 8, 9, 10, 11, 0, 1, 4, 5, 12, 13, 14)
    for i in order:
        copies[i].start()
    copies[2].wait()
    copies[3].wait()
    own = owner_mask(slot_s[...])
    live = column(act_s[...].astype(F32)) > 0.0
    own_b = own.astype(BF16)
    own_ref[...] = own.astype(F32)
    live_own_ref[...] = (own & live).astype(BF16)
    live_ref[...] = jnp.broadcast_to(live.astype(F32), live_ref.shape)
    for st, cw, cb, base, tap, waits in ((bcst_ref, bccw_s, bccb_s, bcbase_ref, bctap_ref, (6, 7, 8)),
                                         (xst_ref, xcw_s, xcb_s, xbase_ref, xtap_ref, (9, 10, 11))):
        for i in waits:
            copies[i].wait()
        weight = cw[...].astype(F32)
        acc = jnp.broadcast_to(cb[...].astype(F32).reshape(1, -1), base.shape)
        for k in range(3):
            acc = acc + jnp.dot(own_b, st[k], preferred_element_type=F32) * weight[k:k + 1]
        base[...] = acc
        tap[...] = weight[3:4]
    for i in (0, 1):
        copies[i].wait()
    gain_ref[...] = gain_s[...].reshape(1, -1)
    ngain_ref[...] = ngain_s[...].reshape(1, -1)
    for i in (4, 5, 12, 13, 14):
        copies[i].wait()


def bc_kernel(n, *refs):
    parts, refs = refs[:n], refs[n:]
    gain_ref, bcw_ref, dtw_ref, base_ref, tap_ref, normed_ref, bc_ref, proj_ref, dt_ref = refs
    bcw, heads = bc_ref.shape[1], dt_ref.shape[1]
    me = lax.axis_index("tp")
    blocks = [p[...] for p in parts]
    width = blocks[0].shape[1]
    for s in range(n):
        pick = blocks[0]
        for k in range(1, n):
            pick = jnp.where(source(me, k, n) == s, blocks[k], pick)
        normed_ref[:, s * width:(s + 1) * width] = pick
    rows = normed_ref[...].astype(F32)
    inv = lax.rsqrt(jnp.mean(rows * rows, axis=1, keepdims=True) + EPS)
    normed = (rows * inv * gain_ref[...]).astype(BF16)
    normed_ref[...] = normed
    side = jnp.concatenate([bcw_ref[...], dtw_ref[...]], axis=0)
    both = lax.dot_general(normed, side, NT, preferred_element_type=F32).astype(BF16)
    dt_ref[...] = both[:, bcw:bcw + heads].astype(F32)
    proj = both[:, :bcw]
    proj_ref[...] = proj
    bc_ref[...] = silu(base_ref[...] + tap_ref[...] * proj.astype(F32)).astype(BF16)


def terms(v):
    high = v.astype(BF16)
    rest = v - high.astype(F32)
    mid = rest.astype(BF16)
    return jnp.concatenate([high, mid, (rest - mid.astype(F32)).astype(BF16)], axis=0)


def in_kernel(hp, normed_ref, xw_ref, zw_ref, base_ref, tap_ref, dt_ref, dtb_ref, rate_ref, skip_ref, own_ref,
              live_ref, xproj_ref, g1_ref, g2_ref, g3_ref, u_ref, dec_ref):
    normed = normed_ref[...]
    xproj = jnp.dot(normed, xw_ref[...], preferred_element_type=F32).astype(BF16)
    xproj_ref[...] = xproj
    seqs, heads = dt_ref.shape
    chans = xw_ref.shape[1]
    live = live_ref[:, :1] > 0.0
    dt = softplus(dt_ref[...] + dtb_ref[...])
    decay = jnp.exp(-dt * jnp.exp(rate_ref[...]))
    spread = (lax.broadcasted_iota(jnp.int32, (heads, chans), 1) // hp
              == lax.broadcasted_iota(jnp.int32, (heads, chans), 0)).astype(BF16)
    rows = 2 * seqs + 16
    wide = jnp.concatenate([dt, decay, jnp.broadcast_to(skip_ref[...], (16, heads))], axis=0)
    wide = jnp.dot(terms(wide), spread, preferred_element_type=F32)
    wide = wide[:rows] + wide[rows:2 * rows] + wide[2 * rows:]
    dt_w, dec_w, skip_w = wide[:seqs], wide[seqs:2 * seqs], wide[2 * seqs:2 * seqs + 1]
    own_b = own_ref[...].astype(BF16)
    kept = lax.dot_general(terms(jnp.where(live, decay, 1.0)), jnp.concatenate([own_b] * 3, axis=0), TN,
                           preferred_element_type=F32)
    for s in range(seqs):
        dec_ref[s] = jnp.broadcast_to(kept[:, s:s + 1], (heads, dec_ref.shape[2]))
    x = silu(base_ref[...] + tap_ref[...] * xproj.astype(F32)).astype(BF16).astype(F32)
    u = dt_w * x
    live_u = jnp.where(live, u, 0.0)
    high = live_u.astype(BF16)
    u_slot = lax.dot_general(jnp.concatenate([own_b, own_b], axis=0),
                             jnp.concatenate([high, (live_u - high.astype(F32)).astype(BF16)], axis=0), TN,
                             preferred_element_type=F32)
    u_ref[...] = u_slot.T
    zproj = jnp.dot(normed, zw_ref[...], preferred_element_type=F32).astype(BF16)
    gate = silu(zproj.astype(F32))
    g1_ref[...] = gate * dec_w
    g2_ref[...] = gate * u
    g3_ref[...] = gate * (skip_w * x)


def hold_kernel(_, __, after_ref, own_ref, out_ref):
    out_ref[...] = own_ref[...]


def early(seqs):
    return range(0, seqs, 2)


def step_slot(s, dst, state_ref, u_ref, dec_ref, b_slot):
    heads = dec_ref.shape[1]
    hp = state_ref.shape[1] // heads
    for h in range(heads):
        rows = slice(h * hp, (h + 1) * hp)
        dst[rows, :] = state_ref[s, rows, :] * dec_ref[s, h:h + 1, :] + u_ref[rows, s:s + 1] * b_slot[s:s + 1]


def out_kernel(n, *refs):
    parts, refs = refs[:n], refs[n:]
    state_ref, own_ref, g1_ref, g2_ref, g3_ref, gain_ref, w_ref, u_ref, dec_ref = refs[:9]
    sends, (own_sum_ref, bcf_ref, next_ref, stage, ring, sems) = refs[9:9 + n - 1], refs[9 + n - 1:]
    me = lax.axis_index("tp")
    seqs = g1_ref.shape[0]
    ns = state_ref.shape[2]
    blocks = [p[...] for p in parts]
    width = blocks[0].shape[1]
    for s in range(n):
        pick = blocks[0]
        for k in range(1, n):
            pick = jnp.where(source(me, k, n) == s, blocks[k], pick)
        bcf_ref[:, s * width:(s + 1) * width] = pick
    own = own_ref[...] > 0.5
    b_rows, c_rows = bcf_ref[:, :ns].astype(F32), bcf_ref[:, ns:].astype(F32)
    dot_bc = jnp.sum(b_rows * c_rows, axis=1, keepdims=True)
    b_slot = lax.dot_general(own_ref[...].astype(BF16), bcf_ref[:, :ns], TN, preferred_element_type=F32)
    y, copies = None, []
    for s in range(0, seqs, 2):
        if s in early(seqs):
            at = len(copies)
            step_slot(s, ring.at[at], state_ref, u_ref, dec_ref, b_slot)
            copies.append(pltpu.make_async_copy(ring.at[at], next_ref.at[s], sems.at[at]))
            copies[-1].start()
        pair = [jnp.where(own[:, t:t + 1], c_rows, 0.0).astype(BF16) for t in (s, s + 1)]
        both = jnp.concatenate([state_ref[s].astype(BF16), state_ref[s + 1].astype(BF16)], axis=1)
        term = lax.dot_general(jnp.concatenate(pair, axis=1), both, NT, preferred_element_type=F32)
        y = term if y is None else y + term
    gated = g1_ref[...] * y + g2_ref[...] * dot_bc + g3_ref[...]
    part_sq = jnp.sum(gated * gated, axis=1, keepdims=True)
    scaled = (gated * gain_ref[...]).astype(BF16)
    sq_high = part_sq.astype(BF16).astype(F32)
    width = w_ref.shape[1] // n
    lane = lax.broadcasted_iota(jnp.int32, (seqs, 128), 1)
    tail = jnp.where(lane == 0, sq_high, jnp.where(lane == 1, part_sq - sq_high, 0.0))
    for d in range(n):
        stage[d, :, :width] = jnp.dot(scaled, w_ref[:, d * width:(d + 1) * width], preferred_element_type=F32)
        stage[d, :, width:] = tail
    own_sum_ref[...] = stage[me]
    for k in range(1, n):
        sends[k - 1][...] = stage[partner(me, k, n)].astype(BF16)
    for copy in copies:
        copy.wait()


def state_kernel(_, state_ref, u_ref, dec_ref, bcf_ref, own_ref, live_own_ref, xst_ref, xproj_ref, bcst_ref, bcproj_ref,
                 next_ref, xnext_ref, bcnext_ref, ring, xkeep, bckeep, sems, pool_sems):
    seqs, chans, ns = state_ref.shape
    b_slot = lax.dot_general(own_ref[...].astype(BF16), bcf_ref[:, :ns], TN, preferred_element_type=F32)
    late = [s for s in range(seqs) if s not in early(seqs)]
    copies = []
    for at, s in enumerate(late):
        step_slot(s, ring.at[at], state_ref, u_ref, dec_ref, b_slot)
        copies.append(pltpu.make_async_copy(ring.at[at], next_ref.at[s], sems.at[at]))
        copies[-1].start()
        if at == len(late) // 2:
            shift_state(xst_ref, xproj_ref[...], live_own_ref[...], xkeep)
            shift_state(bcst_ref, bcproj_ref[...], live_own_ref[...], bckeep)
            pools = [pltpu.make_async_copy(xkeep, xnext_ref, pool_sems.at[0]),
                     pltpu.make_async_copy(bckeep, bcnext_ref, pool_sems.at[1])]
            for pool in pools:
                pool.start()
    for copy in copies + pools:
        copy.wait()


def final_kernel(chans, hid_ref, live_ref, own_ref, *refs):
    got, out_ref = refs[:-1], refs[-1]
    width = hid_ref.shape[1]
    total = own_ref[...]
    for g in got:
        total = total + g[...].astype(F32)
    sq = total[:, width:width + 1] + total[:, width + 1:width + 2]
    inv_out = lax.rsqrt(sq / chans + EPS)
    hidden = hid_ref[...]
    out = (hidden.astype(F32) + inv_out * total[:, :width]).astype(BF16)
    out_ref[...] = jnp.where(live_ref[:, :1] > 0.0, out, hidden)


VM = pl.BlockSpec(memory_space=pltpu.VMEM)
HB = pl.BlockSpec(memory_space=pltpu.HBM)


def call(kernel, name, out, ins, args, outs=None, scratch=(), flops=1e6, moved=1e5, mib=4, alias=None):
    return pl.pallas_call(
        kernel,
        out_shape=out,
        in_specs=ins,
        out_specs=tuple(outs or [VM] * len(out)),
        scratch_shapes=list(scratch),
        input_output_aliases=alias or {},
        name=name,
        compiler_params=pltpu.CompilerParams(vmem_limit_bytes=mib * 2 ** 20),
        cost_estimate=pl.CostEstimate(flops=int(flops), bytes_accessed=int(moved), transcendentals=0),
    )(*args)


def partner(i, k, n):
    return i ^ k if n & (n - 1) == 0 else lax.rem(i + k, n)


def source(i, k, n):
    return i ^ k if n & (n - 1) == 0 else lax.rem(i - k + n, n)


def spread_out(values, n):
    pairs = n & (n - 1) == 0
    return [lax.ppermute(v, "tp", [(i, i ^ k if pairs else (i + k) % n) for i in range(n)])
            for k, v in enumerate(values, 1)]


def shards(hidden, in_gain, z_weight, x_weight, bc_weight, dt_weight, conv_x_weight, conv_x_bias, conv_bc_weight,
           conv_bc_bias, conv_x_state, conv_bc_state, dt_bias, log_rate, skip_gain, ssm_state, norm_gain, out_weight,
           pool_slot, active, *, n):
    seqs, heads, hp, ns = ssm_state.shape
    chans = heads * hp
    width = hidden.shape[1]
    bcw = bc_weight.shape[1]
    row = lambda v: v.reshape(1, -1)
    pinned = lambda v: pltpu.with_memory_space_constraint(v, pltpu.HBM)
    sds = jax.ShapeDtypeStruct
    like = lambda v: sds(v.shape, v.dtype)
    state = ssm_state.reshape(seqs, chans, ns)
    hid, = call(load_kernel, "load", (like(hidden),), [HB], (pinned(hidden),), scratch=[pltpu.SemaphoreType.DMA],
                flops=LEAD, moved=1e5)
    parts = [hid] + spread_out([hid] * (n - 1), n)
    src = (in_gain, norm_gain, row(pool_slot), row(active), bc_weight.T, dt_weight.T, conv_bc_state.transpose(1, 0, 2),
           conv_bc_weight, row(conv_bc_bias), conv_x_state.transpose(1, 0, 2), conv_x_weight, conv_x_bias, row(dt_bias),
           row(log_rate), row(skip_gain))
    held = {i: pltpu.VMEM(src[i].shape, src[i].dtype) for i in (0, 1, 2, 3, 7, 8, 10, 11)}
    (gain, ngain, own, live_own, bcw_v, dtw_v, bcst, bcbase, bctap, xst, xbase, xtap, dtb, rate, skip, live) = call(
        functools.partial(prep_kernel, len(src)), "prep",
        (like(row(in_gain)), like(row(norm_gain)), sds((seqs, seqs), F32), sds((seqs, seqs), BF16), like(src[4]), like(src[5]),
         like(src[6]), sds((seqs, bcw), F32), sds((1, bcw), F32), like(src[9]), sds((seqs, chans), F32),
         sds((1, chans), F32), like(src[12]), like(src[13]), like(src[14]), sds((seqs, 128), F32)),
        [HB] * len(src), tuple(map(pinned, src)), scratch=[*held.values(), pltpu.SemaphoreType.DMA((len(src),))], flops=4e6, moved=1e6)
    normed, bc_own, bcproj, dt = call(
        functools.partial(bc_kernel, n), "bc",
        (sds((seqs, n * width), BF16), sds((seqs, bcw), BF16), sds((seqs, bcw), BF16),
         sds((seqs, heads), F32)),
        [VM] * (n + 5), (*parts, gain, bcw_v, dtw_v, bcbase, bctap), flops=4e6)
    bc_parts = [bc_own] + spread_out([bc_own] * (n - 1), n)
    wide = sds((seqs, chans), F32)
    xproj, g1, g2, g3, u, dec = call(
        functools.partial(in_kernel, hp), "proj",
        (sds((seqs, chans), BF16), wide, wide, wide, sds((chans, seqs), F32), sds((seqs, heads, 128), F32)),
        [VM] * 11, (normed, x_weight, z_weight, xbase, xtap, dt, dtb, rate, skip, own, live))
    own_held, = call(hold_kernel, "hold", (like(own),), [VM] * 4, (state, out_weight, u, own))
    count = len(early(seqs))
    *sends, own_sum, bcf, begun = call(
        functools.partial(out_kernel, n), "out",
        (*[sds((seqs, width + 128), BF16)] * (n - 1), sds((seqs, width + 128), F32), sds((seqs, n * bcw), BF16),
         like(state)),
        [VM] * (n + 9), (*bc_parts, state, own_held, g1, g2, g3, ngain, out_weight, u, dec), outs=(VM,) * (n + 1) + (HB,),
        scratch=[pltpu.VMEM((n, seqs, width + 128), F32), pltpu.VMEM((count, chans, ns), F32),
                 pltpu.SemaphoreType.DMA((count,))], flops=2e8, moved=14e6, mib=12)
    got = spread_out(sends, n)
    fresh, x_next, bc_next = call(
        state_kernel, "state", (like(state), like(xst), like(bcst)), [HB] + [VM] * 10,
        (begun, state, u, dec, bcf, own, live_own, xst, xproj, bcst, bcproj), outs=(HB, HB, HB),
        scratch=[pltpu.VMEM((seqs - count, chans, ns), F32), pltpu.VMEM(xst.shape, BF16), pltpu.VMEM(bcst.shape, BF16),
                 pltpu.SemaphoreType.DMA((seqs - count,)), pltpu.SemaphoreType.DMA((2,))], flops=2e8, moved=14e6, mib=12,
        alias={0: 0})
    layer_out, = call(functools.partial(final_kernel, chans * n), "final", (like(hidden),), [VM] * (n + 2),
                      (hid, live, own_sum, *got))
    return (layer_out, x_next.transpose(1, 0, 2), bc_next.transpose(1, 0, 2), fresh.reshape(ssm_state.shape))


def solution(mesh):
    placed = (
        P(("groups", "dp"), "tp"), P(), P(None, "tp"), P(None, "tp"), P(None, "tp"), P(None, "tp"), P(None, "tp"),
        P("tp"), P(None, "tp"), P("tp"), P(("groups", "dp"), None, "tp"), P(("groups", "dp"), None, "tp"), P("tp"),
        P("tp"), P("tp"), P(("groups", "dp"), "tp", None, None), P("tp"), P("tp", None), P(("groups", "dp"), None),
        P(("groups", "dp")),
    )
    return jax.shard_map(
        functools.partial(shards, n=mesh.shape["tp"]),
        mesh=mesh,
        in_specs=placed,
        out_specs=(P(("groups", "dp"), "tp"), P(("groups", "dp"), None, "tp"), P(("groups", "dp"), None, "tp"),
                   P(("groups", "dp"), "tp", None, None)),
        check_vma=False,
    )
```

```python
import functools
import jax
import jax.numpy as jnp
from jax import lax
from jax.experimental import pallas as pl
from jax.experimental.pallas import tpu as pltpu
from jax.sharding import PartitionSpec as P

F32 = jnp.float32
BF16 = jnp.bfloat16
LEAD = 2e10
NT = (((1,), (1,)), ((), ()))
TN = (((0,), (0,)), ((), ()))
EPS = 1e-05


def column(row):
    n = row.shape[1]
    eye = lax.broadcasted_iota(jnp.int32, (n, n), 0) == lax.broadcasted_iota(jnp.int32, (n, n), 1)
    return jnp.sum(jnp.where(eye, jnp.broadcast_to(row, (n, n)), jnp.zeros((), row.dtype)), axis=1, keepdims=True)


def silu(v):
    return v * (1.0 / (1.0 + jnp.exp(-v)))


def softplus(v):
    return jnp.maximum(v, 0.0) + jnp.log1p(jnp.exp(-jnp.abs(v)))


def owner_mask(slot_row):
    n = slot_row.shape[1]
    slot_col = column(slot_row.astype(F32))
    return slot_col == lax.broadcasted_iota(jnp.int32, (n, n), 1).astype(F32)


def taps(old, current, weight, bias):
    acc = old[0] * weight[0:1]
    acc = acc + old[1] * weight[1:2]
    acc = acc + old[2] * weight[2:3]
    acc = acc + current * weight[3:4]
    return silu(acc + bias).astype(BF16)


def shift_state(st_ref, newest, live_own, next_ref):
    live_slot = lax.dot_general(live_own, jnp.ones(newest.shape, BF16), TN, preferred_element_type=F32) > 0.5
    at_slot = lax.dot_general(live_own, newest, TN, preferred_element_type=F32)
    for k in range(3):
        newer = st_ref[k + 1].astype(F32) if k < 2 else at_slot
        next_ref[k] = jnp.where(live_slot, newer, st_ref[k].astype(F32)).astype(BF16)


def load_kernel(src_ref, dst_ref, sem):
    copy = pltpu.make_async_copy(src_ref, dst_ref, sem)
    copy.start()
    copy.wait()


def prep_kernel(count, xst_ref, bcw_ref, dtw_ref, *refs):
    src, refs = refs[:count], refs[count:]
    (gain_ref, ngain_ref, own_ref, live_own_ref, bcst_ref, bcbase_ref, bctap_ref,
     xbase_ref, xtap_ref, dtb_ref, rate_ref, skip_ref, live_ref, side_ref) = refs[:14]
    gain_s, ngain_s, slot_s, act_s, bccw_s, bccb_s, xcw_s, xcb_s, sems = refs[14:]
    dst = (gain_s, ngain_s, slot_s, act_s, bcst_ref, bccw_s, bccb_s, xcw_s, xcb_s,
           dtb_ref, rate_ref, skip_ref)
    copies = [pltpu.make_async_copy(a, b, sems.at[i]) for i, (a, b) in enumerate(zip(src, dst))]
    order = (2, 3, 4, 5, 6, 7, 8, 0, 1, 9, 10, 11)
    for i in order:
        copies[i].start()
    side = [bcw_ref[...].astype(F32), dtw_ref[...].astype(F32)]
    spare = side_ref.shape[1] - sum(v.shape[0] for v in side)
    if spare:
        side.append(jnp.zeros((spare, side_ref.shape[0]), F32))
    side_ref[...] = jnp.concatenate(side, axis=0).T.astype(BF16)
    copies[2].wait()
    copies[3].wait()
    own = owner_mask(slot_s[...])
    live = column(act_s[...].astype(F32)) > 0.0
    own_b = own.astype(BF16)
    own_ref[...] = own.astype(F32)
    live_own_ref[...] = (own & live).astype(BF16)
    live_ref[...] = jnp.broadcast_to(live.astype(F32), live_ref.shape)
    for st, cw, cb, base, tap, waits in ((bcst_ref, bccw_s, bccb_s, bcbase_ref, bctap_ref, (4, 5, 6)),
                                         (xst_ref, xcw_s, xcb_s, xbase_ref, xtap_ref, (7, 8))):
        for i in waits:
            copies[i].wait()
        weight = cw[...].astype(F32)
        acc = jnp.broadcast_to(cb[...].astype(F32).reshape(1, -1), base.shape)
        for k in range(3):
            acc = acc + jnp.dot(own_b, st[k], preferred_element_type=F32) * weight[k:k + 1]
        base[...] = acc
        tap[...] = weight[3:4]
    for i in (0, 1):
        copies[i].wait()
    gain_ref[...] = gain_s[...].reshape(1, -1)
    ngain_ref[...] = ngain_s[...].reshape(1, -1)
    for i in (9, 10, 11):
        copies[i].wait()


def bc_kernel(n, *refs):
    parts, refs = refs[:n], refs[n:]
    gain_ref, side_ref, base_ref, tap_ref, normed_ref, bc_ref, proj_ref, dt_ref = refs
    bcw, heads = bc_ref.shape[1], dt_ref.shape[1]
    me = lax.axis_index("tp")
    blocks = [p[...] for p in parts]
    width = blocks[0].shape[1]
    for s in range(n):
        pick = blocks[0]
        for k in range(1, n):
            pick = jnp.where(source(me, k, n) == s, blocks[k], pick)
        normed_ref[:, s * width:(s + 1) * width] = pick
    rows = normed_ref[...].astype(F32)
    inv = lax.rsqrt(jnp.mean(rows * rows, axis=1, keepdims=True) + EPS)
    normed = (rows * inv * gain_ref[...]).astype(BF16)
    normed_ref[...] = normed
    both = jnp.dot(normed, side_ref[...], preferred_element_type=F32).astype(BF16)
    dt_ref[...] = both[:, bcw:bcw + heads].astype(F32)
    proj = both[:, :bcw]
    proj_ref[...] = proj
    bc_ref[...] = silu(base_ref[...] + tap_ref[...] * proj.astype(F32)).astype(BF16)


def terms(v):
    high = v.astype(BF16)
    rest = v - high.astype(F32)
    mid = rest.astype(BF16)
    return jnp.concatenate([high, mid, (rest - mid.astype(F32)).astype(BF16)], axis=0)


def in_kernel(hp, normed_ref, xw_ref, zw_ref, base_ref, tap_ref, dt_ref, dtb_ref, rate_ref, skip_ref, own_ref,
              live_ref, xproj_ref, g1_ref, g2_ref, g3_ref, u_ref, dec_ref):
    normed = normed_ref[...]
    xproj = jnp.dot(normed, xw_ref[...], preferred_element_type=F32).astype(BF16)
    xproj_ref[...] = xproj
    seqs, heads = dt_ref.shape
    chans = xw_ref.shape[1]
    live = live_ref[:, :1] > 0.0
    dt = softplus(dt_ref[...] + dtb_ref[...])
    decay = jnp.exp(-dt * jnp.exp(rate_ref[...]))
    spread = (lax.broadcasted_iota(jnp.int32, (heads, chans), 1) // hp
              == lax.broadcasted_iota(jnp.int32, (heads, chans), 0)).astype(BF16)
    rows = 2 * seqs + 16
    wide = jnp.concatenate([dt, decay, jnp.broadcast_to(skip_ref[...], (16, heads))], axis=0)
    wide = jnp.dot(terms(wide), spread, preferred_element_type=F32)
    wide = wide[:rows] + wide[rows:2 * rows] + wide[2 * rows:]
    dt_w, dec_w, skip_w = wide[:seqs], wide[seqs:2 * seqs], wide[2 * seqs:2 * seqs + 1]
    own_b = own_ref[...].astype(BF16)
    kept = lax.dot_general(terms(jnp.where(live, decay, 1.0)), jnp.concatenate([own_b] * 3, axis=0), TN,
                           preferred_element_type=F32)
    for s in range(seqs):
        dec_ref[s] = jnp.broadcast_to(kept[:, s:s + 1], (heads, dec_ref.shape[2]))
    x = silu(base_ref[...] + tap_ref[...] * xproj.astype(F32)).astype(BF16).astype(F32)
    u = dt_w * x
    live_u = jnp.where(live, u, 0.0)
    high = live_u.astype(BF16)
    u_slot = lax.dot_general(jnp.concatenate([own_b, own_b], axis=0),
                             jnp.concatenate([high, (live_u - high.astype(F32)).astype(BF16)], axis=0), TN,
                             preferred_element_type=F32)
    u_ref[...] = u_slot.T
    zproj = jnp.dot(normed, zw_ref[...], preferred_element_type=F32).astype(BF16)
    gate = silu(zproj.astype(F32))
    g1_ref[...] = gate * dec_w
    g2_ref[...] = gate * u
    g3_ref[...] = gate * (skip_w * x)


def hold_kernel(_, __, after_ref, own_ref, out_ref):
    out_ref[...] = own_ref[...]


def early(seqs):
    return range(0, seqs, 2)


def step_slot(s, dst, state_ref, u_ref, dec_ref, b_slot):
    heads = dec_ref.shape[1]
    hp = state_ref.shape[1] // heads
    for h in range(heads):
        rows = slice(h * hp, (h + 1) * hp)
        dst[rows, :] = state_ref[s, rows, :] * dec_ref[s, h:h + 1, :] + u_ref[rows, s:s + 1] * b_slot[s:s + 1]


def out_kernel(n, *refs):
    parts, refs = refs[:n], refs[n:]
    state_ref, own_ref, g1_ref, g2_ref, g3_ref, gain_ref, w_ref, u_ref, dec_ref = refs[:9]
    sends, (own_sum_ref, bcf_ref, next_ref, stage, ring, sems) = refs[9:9 + n - 1], refs[9 + n - 1:]
    me = lax.axis_index("tp")
    seqs = g1_ref.shape[0]
    ns = state_ref.shape[2]
    blocks = [p[...] for p in parts]
    width = blocks[0].shape[1]
    for s in range(n):
        pick = blocks[0]
        for k in range(1, n):
            pick = jnp.where(source(me, k, n) == s, blocks[k], pick)
        bcf_ref[:, s * width:(s + 1) * width] = pick
    own = own_ref[...] > 0.5
    b_rows, c_rows = bcf_ref[:, :ns].astype(F32), bcf_ref[:, ns:].astype(F32)
    dot_bc = jnp.sum(b_rows * c_rows, axis=1, keepdims=True)
    b_slot = lax.dot_general(own_ref[...].astype(BF16), bcf_ref[:, :ns], TN, preferred_element_type=F32)
    y, copies = None, []
    for s in range(0, seqs, 2):
        if s in early(seqs):
            at = len(copies)
            step_slot(s, ring.at[at], state_ref, u_ref, dec_ref, b_slot)
            copies.append(pltpu.make_async_copy(ring.at[at], next_ref.at[s], sems.at[at]))
            copies[-1].start()
        pair = [jnp.where(own[:, t:t + 1], c_rows, 0.0).astype(BF16) for t in (s, s + 1)]
        both = jnp.concatenate([state_ref[s].astype(BF16), state_ref[s + 1].astype(BF16)], axis=1)
        term = lax.dot_general(jnp.concatenate(pair, axis=1), both, NT, preferred_element_type=F32)
        y = term if y is None else y + term
    gated = g1_ref[...] * y + g2_ref[...] * dot_bc + g3_ref[...]
    part_sq = jnp.sum(gated * gated, axis=1, keepdims=True)
    scaled = (gated * gain_ref[...]).astype(BF16)
    sq_high = part_sq.astype(BF16).astype(F32)
    width = w_ref.shape[1] // n
    lane = lax.broadcasted_iota(jnp.int32, (seqs, 128), 1)
    tail = jnp.where(lane == 0, sq_high, jnp.where(lane == 1, part_sq - sq_high, 0.0))
    for d in range(n):
        stage[d, :, :width] = jnp.dot(scaled, w_ref[:, d * width:(d + 1) * width], preferred_element_type=F32)
        stage[d, :, width:] = tail
    own_sum_ref[...] = stage[me]
    for k in range(1, n):
        sends[k - 1][...] = stage[partner(me, k, n)].astype(BF16)
    for copy in copies:
        copy.wait()


def state_kernel(_, state_ref, u_ref, dec_ref, bcf_ref, own_ref, live_own_ref, xst_ref, xproj_ref, bcst_ref, bcproj_ref,
                 next_ref, xnext_ref, bcnext_ref, ring, xkeep, bckeep, sems, pool_sems):
    seqs, chans, ns = state_ref.shape
    b_slot = lax.dot_general(own_ref[...].astype(BF16), bcf_ref[:, :ns], TN, preferred_element_type=F32)
    late = [s for s in range(seqs) if s not in early(seqs)]
    copies = []
    for at, s in enumerate(late):
        step_slot(s, ring.at[at], state_ref, u_ref, dec_ref, b_slot)
        copies.append(pltpu.make_async_copy(ring.at[at], next_ref.at[s], sems.at[at]))
        copies[-1].start()
        if at == len(late) // 2:
            shift_state(xst_ref, xproj_ref[...], live_own_ref[...], xkeep)
            shift_state(bcst_ref, bcproj_ref[...], live_own_ref[...], bckeep)
            pools = [pltpu.make_async_copy(xkeep, xnext_ref, pool_sems.at[0]),
                     pltpu.make_async_copy(bckeep, bcnext_ref, pool_sems.at[1])]
            for pool in pools:
                pool.start()
    for copy in copies + pools:
        copy.wait()


def final_kernel(chans, hid_ref, live_ref, own_ref, *refs):
    got, out_ref = refs[:-1], refs[-1]
    width = hid_ref.shape[1]
    total = own_ref[...]
    for g in got:
        total = total + g[...].astype(F32)
    sq = total[:, width:width + 1] + total[:, width + 1:width + 2]
    inv_out = lax.rsqrt(sq / chans + EPS)
    hidden = hid_ref[...]
    out = (hidden.astype(F32) + inv_out * total[:, :width]).astype(BF16)
    out_ref[...] = jnp.where(live_ref[:, :1] > 0.0, out, hidden)


VM = pl.BlockSpec(memory_space=pltpu.VMEM)
HB = pl.BlockSpec(memory_space=pltpu.HBM)


def call(kernel, name, out, ins, args, outs=None, scratch=(), flops=1e6, moved=1e5, mib=4, alias=None):
    return pl.pallas_call(
        kernel,
        out_shape=out,
        in_specs=ins,
        out_specs=tuple(outs or [VM] * len(out)),
        scratch_shapes=list(scratch),
        input_output_aliases=alias or {},
        name=name,
        compiler_params=pltpu.CompilerParams(vmem_limit_bytes=mib * 2 ** 20),
        cost_estimate=pl.CostEstimate(flops=int(flops), bytes_accessed=int(moved), transcendentals=0),
    )(*args)


def partner(i, k, n):
    return i ^ k if n & (n - 1) == 0 else lax.rem(i + k, n)


def source(i, k, n):
    return i ^ k if n & (n - 1) == 0 else lax.rem(i - k + n, n)


def spread_out(values, n):
    pairs = n & (n - 1) == 0
    return [lax.ppermute(v, "tp", [(i, i ^ k if pairs else (i + k) % n) for i in range(n)])
            for k, v in enumerate(values, 1)]


def shards(hidden, in_gain, z_weight, x_weight, bc_weight, dt_weight, conv_x_weight, conv_x_bias, conv_bc_weight,
           conv_bc_bias, conv_x_state, conv_bc_state, dt_bias, log_rate, skip_gain, ssm_state, norm_gain, out_weight,
           pool_slot, active, *, n):
    seqs, heads, hp, ns = ssm_state.shape
    chans = heads * hp
    width = hidden.shape[1]
    bcw = bc_weight.shape[1]
    row = lambda v: v.reshape(1, -1)
    pinned = lambda v: pltpu.with_memory_space_constraint(v, pltpu.HBM)
    sds = jax.ShapeDtypeStruct
    like = lambda v: sds(v.shape, v.dtype)
    state = ssm_state.reshape(seqs, chans, ns)
    hid, = call(load_kernel, "load", (like(hidden),), [HB], (pinned(hidden),), scratch=[pltpu.SemaphoreType.DMA],
                flops=LEAD, moved=1e5)
    parts = [hid] + spread_out([hid] * (n - 1), n)
    src = (in_gain, norm_gain, row(pool_slot), row(active), conv_bc_state.transpose(1, 0, 2),
           conv_bc_weight, row(conv_bc_bias), conv_x_weight, conv_x_bias, row(dt_bias),
           row(log_rate), row(skip_gain))
    xst = conv_x_state.transpose(1, 0, 2)
    held = {i: pltpu.VMEM(src[i].shape, src[i].dtype) for i in (0, 1, 2, 3, 5, 6, 7, 8)}
    (gain, ngain, own, live_own, bcst, bcbase, bctap, xbase, xtap, dtb, rate, skip, live, side) = call(
        functools.partial(prep_kernel, len(src)), "prep",
        (like(row(in_gain)), like(row(norm_gain)), sds((seqs, seqs), F32), sds((seqs, seqs), BF16),
         like(src[4]), sds((seqs, bcw), F32), sds((1, bcw), F32), sds((seqs, chans), F32),
         sds((1, chans), F32), like(src[9]), like(src[10]), like(src[11]), sds((seqs, 128), F32),
         sds((n * width, -(-(bcw + heads) // 128) * 128), BF16)),
        [VM] * 3 + [HB] * len(src), (xst, bc_weight.T, dt_weight.T, *map(pinned, src)), scratch=[*held.values(), pltpu.SemaphoreType.DMA((len(src),))], flops=4e6, moved=1e6)
    normed, bc_own, bcproj, dt = call(
        functools.partial(bc_kernel, n), "bc",
        (sds((seqs, n * width), BF16), sds((seqs, bcw), BF16), sds((seqs, bcw), BF16),
         sds((seqs, heads), F32)),
        [VM] * (n + 4), (*parts, gain, side, bcbase, bctap), flops=4e6)
    bc_parts = [bc_own] + spread_out([bc_own] * (n - 1), n)
    wide = sds((seqs, chans), F32)
    xproj, g1, g2, g3, u, dec = call(
        functools.partial(in_kernel, hp), "proj",
        (sds((seqs, chans), BF16), wide, wide, wide, sds((chans, seqs), F32), sds((seqs, heads, 128), F32)),
        [VM] * 11, (normed, x_weight, z_weight, xbase, xtap, dt, dtb, rate, skip, own, live))
    own_held, = call(hold_kernel, "hold", (like(own),), [VM] * 4, (state, out_weight, u, own))
    count = len(early(seqs))
    *sends, own_sum, bcf, begun = call(
        functools.partial(out_kernel, n), "out",
        (*[sds((seqs, width + 128), BF16)] * (n - 1), sds((seqs, width + 128), F32), sds((seqs, n * bcw), BF16),
         like(state)),
        [VM] * (n + 9), (*bc_parts, state, own_held, g1, g2, g3, ngain, out_weight, u, dec), outs=(VM,) * (n + 1) + (HB,),
        scratch=[pltpu.VMEM((n, seqs, width + 128), F32), pltpu.VMEM((count, chans, ns), F32),
                 pltpu.SemaphoreType.DMA((count,))], flops=2e8, moved=14e6, mib=12)
    got = spread_out(sends, n)
    fresh, x_next, bc_next = call(
        state_kernel, "state", (like(state), like(xst), like(bcst)), [HB] + [VM] * 10,
        (begun, state, u, dec, bcf, own, live_own, xst, xproj, bcst, bcproj), outs=(HB, HB, HB),
        scratch=[pltpu.VMEM((seqs - count, chans, ns), F32), pltpu.VMEM(xst.shape, BF16), pltpu.VMEM(bcst.shape, BF16),
                 pltpu.SemaphoreType.DMA((seqs - count,)), pltpu.SemaphoreType.DMA((2,))], flops=2e8, moved=14e6, mib=12,
        alias={0: 0})
    layer_out, = call(functools.partial(final_kernel, chans * n), "final", (like(hidden),), [VM] * (n + 2),
                      (hid, live, own_sum, *got))
    return (layer_out, x_next.transpose(1, 0, 2), bc_next.transpose(1, 0, 2), fresh.reshape(ssm_state.shape))


def solution(mesh):
    placed = (
        P(("groups", "dp"), "tp"), P(), P(None, "tp"), P(None, "tp"), P(None, "tp"), P(None, "tp"), P(None, "tp"),
        P("tp"), P(None, "tp"), P("tp"), P(("groups", "dp"), None, "tp"), P(("groups", "dp"), None, "tp"), P("tp"),
        P("tp"), P("tp"), P(("groups", "dp"), "tp", None, None), P("tp"), P("tp", None), P(("groups", "dp"), None),
        P(("groups", "dp")),
    )
    return jax.shard_map(
        functools.partial(shards, n=mesh.shape["tp"]),
        mesh=mesh,
        in_specs=placed,
        out_specs=(P(("groups", "dp"), "tp"), P(("groups", "dp"), None, "tp"), P(("groups", "dp"), None, "tp"),
                   P(("groups", "dp"), "tp", None, None)),
        check_vma=False,
    )
```
